32 devices in a mesh: dp: 4 (over x, core), fsdp: 8 (over z, y).
Axes of the slice: x: 2, y: 2, z: 4, core: 2. Of those that a mesh axis runs over, the one named last changes fastest.
Arguments:
- tokens: bfloat16 [32768, 768], P(('dp', 'fsdp')), may hold values from -6 to 6
- segment_ids: int32 [32768], P(('dp', 'fsdp')), may hold values from 0 to 543, as said below
- live_mask: int32 [32768], P(('dp', 'fsdp')), may hold values from 0 to 1, as said below
- cotangent: bfloat16 [32768, 768], P(('dp', 'fsdp')), may hold values from -6 to 6
- first_gain: bfloat16 [768], P(('dp', 'fsdp')), may hold values from 0.099609375 to 1.8984375
- first_shift: bfloat16 [768], P(('dp', 'fsdp')), may hold values from -4 to 4
- qkv_weight: bfloat16 [768, 2304], P(('dp', 'fsdp')), may hold values from -0.21875 to 0.21875
- query_bias: bfloat16 [768], P(('dp', 'fsdp')), may hold values from -4 to 4
- value_bias: bfloat16 [768], P(('dp', 'fsdp')), may hold values from -4 to 4
- proj_weight: bfloat16 [768, 768], P(('dp', 'fsdp')), may hold values from -1.75 to 1.75
- proj_bias: bfloat16 [768], P(('dp', 'fsdp')), may hold values from -4 to 4
- second_gain: bfloat16 [768], P(('dp', 'fsdp')), may hold values from 0.099609375 to 1.8984375
- second_shift: bfloat16 [768], P(('dp', 'fsdp')), may hold values from -4 to 4
- inner_weight: bfloat16 [768, 3072], P(('dp', 'fsdp')), may hold values from -0.21875 to 0.21875
- inner_bias: bfloat16 [3072], P(('dp', 'fsdp')), may hold values from -4 to 4
- outer_weight: bfloat16 [3072, 768], P(('dp', 'fsdp')), may hold values from -0.21875 to 0.21875
- outer_bias: bfloat16 [768], P(('dp', 'fsdp')), may hold values from -4 to 4
Outputs:
- layer_out: bfloat16 [32768, 768], P(('dp', 'fsdp'))
- grad_tokens: bfloat16 [32768, 768], P(('dp', 'fsdp'))
- grad_first_gain: float32 [768], P(('dp', 'fsdp'))
- grad_first_shift: float32 [768], P(('dp', 'fsdp'))
- grad_qkv: float32 [768, 2304], P(('dp', 'fsdp'))
- grad_query_bias: float32 [768], P(('dp', 'fsdp'))
- grad_value_bias: float32 [768], P(('dp', 'fsdp'))
- grad_proj: float32 [768, 768], P(('dp', 'fsdp'))
- grad_proj_bias: float32 [768], P(('dp', 'fsdp'))
- grad_second_gain: float32 [768], P(('dp', 'fsdp'))
- grad_second_shift: float32 [768], P(('dp', 'fsdp'))
- grad_inner: float32 [768, 3072], P(('dp', 'fsdp'))
- grad_inner_bias: float32 [3072], P(('dp', 'fsdp'))
- grad_outer: float32 [3072, 768], P(('dp', 'fsdp'))
- grad_outer_bias: float32 [768], P(('dp', 'fsdp'))
The draws below stay inside these ranges and needn't reach their ends.
Inputs may be any that keep to these rules, and one draw needn't show every extreme that they name: `segment_ids`: each aligned block of 1024 rows (the rows of one device) holds whole examples, each a run of consecutive rows with an id that no other example or block uses: image-text examples of 228 rows and text examples of 64 rows, in any order and number; the block's remaining rows at its end, 64 or more of them, share one further id of their own. `live_mask`: in an image-text example its 196 patch rows and its first 1 to 32 text rows are 1, in a text example its first 1 to 64 rows; all other rows are 0.
All inputs are finite; a program needn't handle non-finite values.
Results may differ from the reference program's by a relative error of at most 0.012.
Values may be sent and summed in bfloat16 or wider, within the bound.
A program may use at most 256 MiB of HBM per device.

```python
import jax
import jax.numpy as jnp
from jax import lax

D = 768
HEADS = 12
HEAD = 64
FF = 3072
IMG = 196
TXT = 32
PLAIN = 64
ROWS = 1024
BLOCK = 512
TOKENS = 32768


def packing_plan(key):
    device_count = TOKENS // ROWS
    slot_count = ROWS // PLAIN
    example_kind = jax.random.randint(jax.random.fold_in(key, 11), (device_count, slot_count), 0, 2)
    fill_limit = jax.random.randint(jax.random.fold_in(key, 12), (device_count, 1), ROWS // 2, ROWS - PLAIN + 1)
    lengths = jnp.where(example_kind == 1, IMG + TXT, PLAIN)
    end_rows = jnp.cumsum(lengths, axis=1)
    start_rows = end_rows - lengths
    fitting = end_rows <= fill_limit
    text_rows = jnp.where(example_kind == 1, TXT, PLAIN)
    spoken = jax.random.randint(jax.random.fold_in(key, 13), (device_count, slot_count), 0, 1 << 20) % text_rows + 1
    leading = jnp.where(example_kind == 1, IMG, 0)
    row_index = jnp.arange(ROWS)
    inside = (row_index[None, None, :] >= start_rows[:, :, None]) & (row_index[None, None, :] < end_rows[:, :, None]) & fitting[:, :, None]
    inside_int = inside.astype(jnp.int32)
    covered = jnp.sum(inside_int, axis=1)
    slot_index = jnp.sum(inside_int * jnp.arange(slot_count)[None, :, None], axis=1) + (1 - covered) * slot_count
    offsets = row_index[None, :] - jnp.sum(inside_int * start_rows[:, :, None], axis=1)
    live_limit = jnp.sum(inside_int * (leading + spoken)[:, :, None], axis=1)
    live_rows = covered * (offsets < live_limit).astype(jnp.int32)
    segment = jnp.arange(device_count)[:, None] * (slot_count + 1) + slot_index
    return (segment.reshape(-1).astype(jnp.int32), live_rows.reshape(-1).astype(jnp.int32))


def draw_segment_ids(key, part):
    return packing_plan(key)[0]


def draw_live_mask(key, part):
    return packing_plan(key)[1]


def spiked(values, rng, source, target, shards_of, factor):
    owner, partner = [(jnp.arange(values.shape[dim]) // (values.shape[dim] // shards_of)).reshape([-1 if axis == dim else 1 for axis in range(values.ndim)]) for dim in (source, target)]
    chosen = jax.random.permutation(rng, shards_of)[partner]
    strong = (owner == chosen) | (owner == (partner + shards_of // 2) % shards_of)
    return jnp.where(strong, factor * values, values)


def steps_of(key, shape, cuts, low, top_value):
    def one(axis_at, blocks):
        steps = jax.random.uniform(jax.random.fold_in(jax.random.fold_in(key, 6), axis_at), (blocks,), jnp.float32, low / len(cuts), top_value / len(cuts))
        return jnp.repeat(jnp.exp(steps), shape[axis_at] // blocks).reshape((-1,) + (1,) * (len(shape) - axis_at - 1))

    loudness = one(*cuts[0])
    for cut in cuts[1:]:
        loudness = loudness * one(*cut)
    return loudness


def bell_draw(own_key, extent, scale, reach, pieces=(), kind=jnp.bfloat16):
    entries = jax.random.normal(own_key, extent, jnp.float32) * scale
    if len(pieces) > 0:
        entries = steps_of(own_key, extent, pieces, -0.22, 0.18) * entries
    return jnp.clip(entries, min=-reach, max=reach).astype(kind)


def heavy_noise(rng, extent, deviation, reach, shards, heavy, held_as=jnp.bfloat16):
    entries = deviation * jax.random.normal(rng, extent, jnp.float32)
    if shards:
        entries = entries * steps_of(rng, extent, shards, -0.22, 0.18)
    return jnp.clip(spiked(entries, jax.random.fold_in(rng, 3), *heavy), -reach, reach).astype(held_as)


def setup_inputs(seed: int = 0) -> dict:
    key_of = jax.random.split(jax.random.key(seed), 18)
    return {
        "tokens": heavy_noise(key_of[0], (TOKENS, D), 1.0, 6.0, ((0, 32),), (0, 1, 32, 2.75)),
        "segment_ids": draw_segment_ids(jax.random.fold_in(key_of[17], 71), 0),
        "live_mask": draw_live_mask(jax.random.fold_in(key_of[17], 71), 0),
        "cotangent": heavy_noise(key_of[3], (TOKENS, D), 1.0, 6.0, ((0, 32),), (0, 1, 32, 2.75)),
        "first_gain": jnp.clip(1.0 + 0.18 * jax.random.normal(key_of[4], (D,), jnp.float32), 0.099609375, 1.8984375).astype(jnp.bfloat16),
        "first_shift": bell_draw(key_of[5], (D,), 0.3, 4.0, ((0, 32),)),
        "qkv_weight": bell_draw(key_of[6], (D, 3 * D), D ** -0.5, 0.21875, ((0, 32),)),
        "query_bias": bell_draw(key_of[7], (D,), 0.3, 4.0, ((0, 32),)),
        "value_bias": bell_draw(key_of[8], (D,), 0.3, 4.0, ((0, 32),)),
        "proj_weight": bell_draw(key_of[9], (D, D), (D // 64) ** -0.5, 1.75, ((0, 32),)),
        "proj_bias": bell_draw(key_of[10], (D,), 0.3, 4.0, ((0, 32),)),
        "second_gain": jnp.clip(1.0 + 0.18 * jax.random.normal(key_of[11], (D,), jnp.float32), 0.099609375, 1.8984375).astype(jnp.bfloat16),
        "second_shift": bell_draw(key_of[12], (D,), 0.3, 4.0, ((0, 32),)),
        "inner_weight": bell_draw(key_of[13], (D, FF), D ** -0.5, 0.21875, ((0, 32),)),
        "inner_bias": bell_draw(key_of[14], (FF,), 0.3, 4.0, ((0, 32),)),
        "outer_weight": bell_draw(key_of[15], (FF, D), (FF // 4) ** -0.5, 0.21875, ((0, 32),)),
        "outer_bias": bell_draw(key_of[16], (D,), 0.3, 4.0, ((0, 32),)),
    }


epsilon = 1e-06
tanh_scale = 0.7978845608028654

@jax.custom_vjp
def low(v):
    return lax.optimization_barrier(v.astype(jnp.bfloat16)).astype(jnp.float32)

@jax.custom_vjp
def low_back(v):
    return v

def low_keep(v):
    return (low(v), None)

def low_pass(kept, grad):
    return (grad,)

def back_keep(v):
    return (v, None)

def back_low(kept, grad):
    return (low(grad),)
low.defvjp(low_keep, low_pass)
low_back.defvjp(back_keep, back_low)

def matmul(first_matrix, second_matrix):
    return jnp.dot(first_matrix, second_matrix, precision=lax.Precision.HIGHEST)

def normed(values, gain_row, shift_row):
    center = values - lax.optimization_barrier(jnp.mean(values, axis=-1, keepdims=True))
    spread = lax.optimization_barrier(jnp.mean(center * center, axis=-1, keepdims=True))
    return center * lax.rsqrt(spread + epsilon) * gain_row + shift_row

def gelu_tanh(values):
    return 0.5 * values * (1.0 + jnp.tanh(tanh_scale * (values + 0.044715 * values * values * values)))

def attend_block(query_heads, key_heads, value_heads, segment_rows, live_rows, first_row):
    query_part = lax.dynamic_slice_in_dim(query_heads, first_row, BLOCK, 0)
    segment_part = lax.dynamic_slice_in_dim(segment_rows, first_row, BLOCK, 0)
    query_index = first_row + jnp.arange(BLOCK, dtype=jnp.int32)
    key_index = jnp.arange(ROWS, dtype=jnp.int32)
    allowed = (segment_part[:, None] == segment_rows[None, :]) & ((live_rows[None, :] == 1) | (query_index[:, None] == key_index[None, :]))
    scores = jnp.einsum('qhe,khe->hqk', query_part, key_heads, precision=lax.Precision.HIGHEST) * HEAD ** (-0.5)
    scores = low_back(scores)
    masked = jnp.where(allowed[None], scores, -1e+30)
    row_peak = lax.optimization_barrier(jnp.max(masked, axis=-1, keepdims=True))
    weights = jnp.where(allowed[None], jnp.exp(masked - row_peak), 0.0)
    probability = low(weights / lax.optimization_barrier(jnp.sum(weights, axis=-1, keepdims=True)))
    return jnp.einsum('hqk,khe->qhe', probability, value_heads, precision=lax.Precision.HIGHEST)

def layer_block(tokens, segment_rows, live_rows, params):
    first_gain, first_shift, qkv_weight, query_bias, value_bias, proj_weight, proj_bias, second_gain, second_shift, inner_weight, inner_bias, outer_weight, outer_bias = params
    hidden_one = low(normed(tokens, first_gain, first_shift))
    mixed = matmul(hidden_one, qkv_weight)
    query_heads = low_back(low(mixed[:, :D] + query_bias)).reshape(ROWS, HEADS, HEAD)
    key_heads = low_back(low(mixed[:, D:2 * D])).reshape(ROWS, HEADS, HEAD)
    value_heads = low_back(low(mixed[:, 2 * D:] + value_bias)).reshape(ROWS, HEADS, HEAD)
    block_fn = jax.checkpoint(attend_block)
    first_rows = jnp.arange(ROWS // BLOCK, dtype=jnp.int32) * BLOCK
    attended = lax.map(lambda first_row: block_fn(query_heads, key_heads, value_heads, segment_rows, live_rows, first_row), first_rows)
    attended = low_back(low(attended.reshape(ROWS, D)))
    resid = tokens + low_back(matmul(attended, proj_weight) + proj_bias)
    hidden_two = low(normed(resid, second_gain, second_shift))
    pre = low_back(matmul(hidden_two, inner_weight) + inner_bias)
    act = low(gelu_tanh(pre))
    return resid + matmul(act, outer_weight) + outer_bias

def layer_all(tokens, segment_ids, live_mask, params):
    token_blocks = tokens.reshape(-1, ROWS, D)
    segment_blocks = segment_ids.reshape(-1, ROWS)
    live_blocks = live_mask.reshape(-1, ROWS)
    block_step = jax.checkpoint(layer_block)

    def scan_step(carried, item):
        return (carried, block_step(item[0], item[1], item[2], params))
    carried, outputs = lax.scan(scan_step, jnp.zeros((), jnp.float32), (token_blocks, segment_blocks, live_blocks))
    return outputs.reshape(-1, D)

def reference(tokens, segment_ids, live_mask, cotangent, first_gain, first_shift, qkv_weight, query_bias, value_bias, proj_weight, proj_bias, second_gain, second_shift, inner_weight, inner_bias, outer_weight, outer_bias):
    params = tuple((item.astype(jnp.float32) for item in (first_gain, first_shift, qkv_weight, query_bias, value_bias, proj_weight, proj_bias, second_gain, second_shift, inner_weight, inner_bias, outer_weight, outer_bias)))

    def forward(tokens_wide, *param_list):
        return layer_all(tokens_wide, segment_ids, live_mask, param_list)
    output, pullback = jax.vjp(forward, tokens.astype(jnp.float32), *params)
    grads = pullback(cotangent.astype(jnp.float32))
    return (output.astype(jnp.bfloat16), grads[0].astype(jnp.bfloat16), grads[1], grads[2], grads[3], grads[4], grads[5], grads[6], grads[7], grads[8], grads[9], grads[10], grads[11], grads[12], grads[13])
```

```python
import jax
import jax.numpy as jnp
from jax import lax
from jax.experimental import pallas as pl
from jax.experimental.pallas import tpu as pltpu
from jax.sharding import PartitionSpec as P

D = 768
HEADS = 12
HEAD = 64
F32 = jnp.float32
BF16 = jnp.bfloat16
MESH = pl.DeviceIdType.MESH
AXES = ("dp", "fsdp")
epsilon = 1e-06
tanh_scale = 0.7978845608028654


def place():
    dp, fs = lax.axis_index("dp"), lax.axis_index("fsdp")
    return dp // 2, dp % 2, fs // 2, fs % 2

def device(x, c, z, y):
    return (x * 2 + c, z * 2 + y)

def peers(at):
    x, c, z, y = at
    return [device(x, c, (z + 1) % 4, y), device(x, c, (z + 2) % 4, y), device(x, c, (z + 3) % 4, y),
            device(x, c, z, 1 - y), device(1 - x, c, z, y), device(x, 1 - c, z, y)]

def greet(at):
    barrier = pltpu.get_barrier_semaphore()
    for peer in peers(at):
        pl.semaphore_signal(barrier, inc=1, device_id=peer, device_id_type=MESH)
    pl.semaphore_wait(barrier, 6)

def remote(src, dst, send, recv, to):
    return pltpu.make_async_remote_copy(src_ref=src, dst_ref=dst, send_sem=send, recv_sem=recv, device_id=to, device_id_type=MESH)

class Gather:
    def __init__(self, unit, at, src, out, cols, y_first, send, recv, local):
        x, c, z, y = at
        self.copies = []
        col = lambda ref: ref.at[:, cols]
        dst = lambda *i: out.at[i[0], i[1], i[2], i[3], :, cols]
        s = lambda i: (send.at[unit, i], recv.at[unit, i])
        own = out.at[x, c, z, y, :, cols]
        self.keep = pltpu.make_async_copy(src.at[:, cols], own, local.at[unit])
        self.z = [remote(src.at[:, cols], own, *s(d), device(x, c, (z + d + 1) % 4, y)) for d in range(3)]
        line = out.at[x, c, :, y, :, cols]
        core = device(x, 1 - c, z, y)
        ydev, xdev = device(x, c, z, 1 - y), device(1 - x, c, z, y)
        if y_first:
            first, second = ydev, xdev
            got1 = out.at[x, c, :, 1 - y, :, cols]
            held = out.at[x, c, :, :, :, cols]
            got2 = out.at[1 - x, c, :, :, :, cols]
        else:
            first, second = xdev, ydev
            got1 = out.at[1 - x, c, :, y, :, cols]
            held = out.at[:, c, :, y, :, cols]
            got2 = out.at[:, c, :, 1 - y, :, cols]
        self.one = remote(line, line, *s(3), first)
        self.two = remote(held, held, *s(4), second)
        self.core = [remote(line, line, *s(5), core), remote(got1, got1, *s(6), core), remote(got2, got2, *s(7), core)]
    def start(self):
        self.keep.start()
        for copy in self.z:
            copy.start()
    def step1(self):
        self.keep.wait()
        for copy in self.z:
            copy.wait_recv()
        self.one.start()
        self.core[0].start()
    def step2(self):
        self.one.wait_recv()
        self.two.start()
        self.core[1].start()
    def step3(self):
        self.two.wait_recv()
        self.core[2].start()
    def arrive(self):
        for copy in self.core:
            copy.wait_recv()
    def sent(self):
        for copy in self.z + [self.one, self.two] + self.core:
            copy.wait_send()

DEPTH = 3
UNITS = ((0, 0, 1152, True), (0, 1152, 2304, False), (4, 0, 128, True), (1, 0, 384, True), (1, 384, 768, False),
         (2, 0, 1536, True), (2, 1536, 3072, False), (3, 0, 384, True), (3, 384, 768, False))

def gather_kernel(*refs):
    srcs, outs, (send, recv, local) = refs[:5], refs[5:10], refs[10:]
    at = place()
    greet(at)
    units = [Gather(u, at, srcs[k], outs[k], slice(a, b), yf, send, recv, local) for u, (k, a, b, yf) in enumerate(UNITS)]
    n = len(units)
    for u in units[:DEPTH]: u.start()
    for t in range(n + 4):
        for name, lag in (("step1", 0), ("step2", 1), ("step3", 2), ("arrive", 3)):
            i = t - lag
            if 0 <= i < n:
                getattr(units[i], name)()
                if name == "step1" and i + DEPTH < n: units[i + DEPTH].start()
    for u in units: u.sent()

def gather(qkv, proj, inner, outer, vec):
    ins = (qkv, proj, inner, outer, vec)
    out = pl.pallas_call(gather_kernel,
        out_shape=[jax.ShapeDtypeStruct((2, 2, 4, 2) + a.shape, a.dtype) for a in ins],
        in_specs=[pl.BlockSpec(memory_space=pltpu.VMEM)] * 5,
        out_specs=[pl.BlockSpec(memory_space=pl.ANY)] * 5,
        scratch_shapes=[pltpu.SemaphoreType.DMA((len(UNITS), 8)), pltpu.SemaphoreType.DMA((len(UNITS), 8)), pltpu.SemaphoreType.DMA((len(UNITS),))],
        compiler_params=pltpu.CompilerParams(collective_id=0, has_side_effects=True, vmem_limit_bytes=60 * 2**20),
        )(*ins)
    return tuple(o.reshape(-1, a.shape[1]) for o, a in zip(out, ins))

class Scatter:
    def __init__(self, unit, at, src, out, cols, x_first, bufs, send, recv, local):
        x, c, z, y = at
        self.at, self.out, self.cols, self.x_first = at, out, cols, x_first
        s = lambda i: (send.at[unit, i], recv.at[unit, i])
        self.mine, self.r0, self.r1, self.r2, self.r3 = mine, r0, r1, r2, r3 = bufs
        grad = lambda cc: src.at[:, cc, :, :, :, cols]
        core, ydev, xdev = device(x, 1 - c, z, y), device(x, c, z, 1 - y), device(1 - x, c, z, y)
        self.load = pltpu.make_async_copy(grad(c), mine, local.at[unit])
        self.c0 = remote(grad(1 - c), r0, *s(0), core)
        if x_first:
            self.c1 = remote(mine.at[1 - x], r1, *s(1), xdev)
            self.c2 = remote(mine.at[x, :, 1 - y], r2, *s(2), ydev)
        else:
            self.c1 = remote(mine.at[:, :, 1 - y], r1, *s(1), ydev)
            self.c2 = remote(mine.at[1 - x, :, y], r2, *s(2), xdev)
        self.z = [remote(mine.at[x, (z + d + 1) % 4, y], r3.at[d], *s(3 + d), device(x, c, (z + d + 1) % 4, y)) for d in range(3)]
    def start(self):
        self.c0.start()
        self.load.start()
    def add(self, target, other):
        target[...] = (target[...].astype(F32) + other[...].astype(F32)).astype(BF16)
    def step1(self):
        self.load.wait()
        self.c0.wait_recv()
        @pl.loop(0, 16)
        def _(j):
            i = (j // 8, (j // 2) % 4, j % 2)
            self.add(self.mine.at[i], self.r0.at[i])
        self.c1.start()
    def step2(self):
        x, c, z, y = self.at
        self.c1.wait_recv()
        @pl.loop(0, 8)
        def _(j):
            if self.x_first:
                self.add(self.mine.at[x, j // 2, j % 2], self.r1.at[j // 2, j % 2])
            else:
                self.add(self.mine.at[j // 4, j % 4, y], self.r1.at[j // 4, j % 4])
        self.c2.start()
    def step3(self):
        x, c, z, y = self.at
        self.c2.wait_recv()
        @pl.loop(0, 4)
        def _(j):
            self.add(self.mine.at[x, j, y], self.r2.at[j])
        for copy in self.z: copy.start()
    def finish(self):
        x, c, z, y = self.at
        for copy in self.z: copy.wait_recv()
        total = self.mine[x, z, y].astype(F32)
        for d in range(3):
            total = total + self.r3[d].astype(F32)
        self.out[:, self.cols] = total
    def sent(self):
        for copy in [self.c0, self.c1, self.c2] + self.z:
            copy.wait_send()

R_UNITS = ((3, 0, 384, True), (3, 384, 768, False), (2, 0, 1536, True), (2, 1536, 3072, False), (1, 0, 384, True), (1, 384, 768, False),
         (0, 0, 1152, True), (0, 1152, 2304, False), (4, 0, 128, True))
R_DEPTH = 2

def scatter_kernel(*refs):
    srcs, outs, (send, recv, local), bufs = refs[:5], refs[5:10], refs[10:13], refs[13:]
    at = place()
    greet(at)
    units = [Scatter(u, at, srcs[k], outs[k], slice(a, b), xf, bufs[5 * u:5 * u + 5], send, recv, local) for u, (k, a, b, xf) in enumerate(R_UNITS)]
    n = len(units)
    for u in units[:R_DEPTH]: u.start()
    for t in range(n + 4):
        for name, lag in (("step1", 0), ("step2", 1), ("step3", 2), ("finish", 3)):
            i = t - lag
            if 0 <= i < n:
                getattr(units[i], name)()
                if name == "step1" and i + R_DEPTH < n: units[i + R_DEPTH].start()
    for u in units: u.sent()

def scatter(*ins):
    ins = [a.reshape(2, 2, 4, 2, -1, a.shape[1]) for a in ins]
    bufs = []
    for k, a, b, xf in R_UNITS:
        block = (ins[k].shape[4], b - a)
        for lead in ((2, 4, 2), (2, 4, 2), (4, 2) if xf else (2, 4), (4,), (3,)):
            bufs.append(pltpu.VMEM(lead + block, BF16))
    return pl.pallas_call(scatter_kernel,
        out_shape=[jax.ShapeDtypeStruct(a.shape[4:], F32) for a in ins],
        in_specs=[pl.BlockSpec(memory_space=pl.ANY)] * 5,
        out_specs=[pl.BlockSpec(memory_space=pltpu.VMEM)] * 5,
        scratch_shapes=[pltpu.SemaphoreType.DMA((len(R_UNITS), 6)), pltpu.SemaphoreType.DMA((len(R_UNITS), 6)), pltpu.SemaphoreType.DMA((len(R_UNITS),))] + bufs,
        compiler_params=pltpu.CompilerParams(collective_id=1, has_side_effects=True, vmem_limit_bytes=60 * 2**20),
        )(*ins)
BQ = 128
REACH = 2
NEG = -1e30

def window(block, blocks):
    return max(0, block - REACH), min(blocks, block + REACH + 1)

def nn(a, b):
    return lax.dot_general(a, b, (((1,), (0,)), ((), ())), preferred_element_type=F32)

def fill_bias(seg_row, key_code, bias_ref, blocks):
    slot = 0
    for b in range(blocks):
        low, high = window(b, blocks)
        q = seg_row[:, b * BQ:(b + 1) * BQ]
        for kb in range(low, high):
            code = key_code[kb * BQ:(kb + 1) * BQ, :]
            ok = code == q
            if kb == b:
                ok = ok | (lax.broadcasted_iota(jnp.int32, (BQ, BQ), 0) == lax.broadcasted_iota(jnp.int32, (BQ, BQ), 1))
            bias_ref[slot * BQ:(slot + 1) * BQ, :] = jnp.where(ok, 0.0, NEG)
            slot += 1

def slots_before(b, blocks):
    return sum(window(i, blocks)[1] - window(i, blocks)[0] for i in range(b))

def beside(top, low_rows):
    zero = jnp.zeros_like(top)
    return jnp.concatenate([jnp.where(low_rows, top, zero), jnp.where(low_rows, zero, top)], axis=1)

def fwd_kernel(seg_ref, code_ref, q_ref, k_ref, v_ref, o_ref, lse_ref, bias_ref):
    rows = q_ref.shape[0]
    blocks = rows // BQ
    @pl.when(pl.program_id(0) == 0)
    def _():
        fill_bias(seg_ref[...], code_ref[...], bias_ref, blocks)
    low_rows = lax.broadcasted_iota(jnp.int32, (2 * HEAD, BQ), 0) < HEAD
    vt = v_ref[...].T
    for b in range(blocks):
        low, high = window(b, blocks)
        at = slots_before(b, blocks)
        n = high - low
        qt = (q_ref[b * BQ:(b + 1) * BQ, :] * HEAD ** -0.5).T
        s = nn(k_ref[low * BQ:high * BQ, :], beside(qt, low_rows))
        bias = bias_ref[at * BQ:(at + n) * BQ, :]
        outs = []
        for h in range(2):
            sh = s[:, h * BQ:(h + 1) * BQ] + bias
            peak = jnp.max(sh, axis=0, keepdims=True)
            e = jnp.exp(sh - peak)
            total = jnp.sum(e, axis=0, keepdims=True)
            lse_ref[0, b:b + 1, h * BQ:(h + 1) * BQ] = peak + jnp.log(total)
            outs.append((e.astype(BF16), total))
        ot = nn(vt[:, low * BQ:high * BQ], jnp.concatenate([outs[0][0], outs[1][0]], axis=1))
        ot = jnp.concatenate([ot[:HEAD, :BQ] / outs[0][1], ot[HEAD:, BQ:] / outs[1][1]], axis=0)
        o_ref[b * BQ:(b + 1) * BQ, :] = ot.T.astype(BF16)

def bwd_kernel(seg_ref, code_ref, q_ref, k_ref, v_ref, o_ref, do_ref, lse_ref, dq_ref, dk_ref, dv_ref, bias_ref, dk_acc, dv_acc):
    rows = q_ref.shape[0]
    blocks = rows // BQ
    @pl.when(pl.program_id(0) == 0)
    def _():
        fill_bias(seg_ref[...], code_ref[...], bias_ref, blocks)
    low_rows = lax.broadcasted_iota(jnp.int32, (2 * HEAD, BQ), 0) < HEAD
    low_cols = lax.broadcasted_iota(jnp.int32, (BQ, 2 * HEAD), 1) < HEAD
    kt = k_ref[...].T
    dk_acc[...] = jnp.zeros_like(dk_acc)
    dv_acc[...] = jnp.zeros_like(dv_acc)
    def stack(x):
        zero = jnp.zeros_like(x)
        return jnp.concatenate([jnp.where(low_cols, x, zero), jnp.where(low_cols, zero, x)], axis=0)
    for b in range(blocks):
        low, high = window(b, blocks)
        at = slots_before(b, blocks)
        n = high - low
        here = slice(b * BQ, (b + 1) * BQ)
        q = q_ref[here, :] * HEAD ** -0.5
        do = do_ref[here, :]
        dprod = (do.astype(F32) * o_ref[here, :].astype(F32)).T
        keys = slice(low * BQ, high * BQ)
        s = nn(k_ref[keys, :], beside(q.T, low_rows))
        dp = nn(v_ref[keys, :], beside(do.T, low_rows))
        bias = bias_ref[at * BQ:(at + n) * BQ, :]
        ps, ds = [], []
        for h in range(2):
            cols = slice(h * BQ, (h + 1) * BQ)
            p = jnp.exp(s[:, cols] + bias - lse_ref[0, b:b + 1, cols])
            delta = jnp.sum(dprod[h * HEAD:(h + 1) * HEAD], axis=0, keepdims=True)
            ds.append((p * (dp[:, cols] - delta)).astype(BF16))
            ps.append(p.astype(BF16))
        p2 = jnp.concatenate(ps, axis=1)
        ds2 = jnp.concatenate(ds, axis=1)
        dv_acc[keys, :] += nn(p2, stack(do))
        dk_acc[keys, :] += nn(ds2, stack(q))
        dqt = nn(kt[:, keys], ds2)
        dqt = jnp.concatenate([dqt[:HEAD, :BQ], dqt[HEAD:, BQ:]], axis=0) * HEAD ** -0.5
        dq_ref[here, :] = dqt.T.astype(BF16)
    dk_ref[...] = dk_acc[...].astype(BF16)
    dv_ref[...] = dv_acc[...].astype(BF16)

def specs(rows):
    col = lambda off: pl.BlockSpec((rows, 2 * HEAD), lambda p: (0, p + off))
    full = lambda s: pl.BlockSpec(s, lambda p: (0,) * len(s))
    return col, full

def attn_fwd(seg_row, code_col, mixed):
    rows = mixed.shape[0]; width = mixed.shape[1] // 3; pairs = width // (2 * HEAD); blocks = rows // BQ
    col, full = specs(rows)
    return pl.pallas_call(fwd_kernel, grid=(pairs,),
        in_specs=[full((1, rows)), full((rows, 1)), col(0), col(pairs), col(2 * pairs)],
        out_specs=[col(0), pl.BlockSpec((1, blocks, 2 * BQ), lambda p: (p, 0, 0))],
        out_shape=[jax.ShapeDtypeStruct((rows, width), BF16), jax.ShapeDtypeStruct((pairs, blocks, 2 * BQ), F32)],
        scratch_shapes=[pltpu.VMEM((slots_before(blocks, blocks) * BQ, BQ), F32)],
        compiler_params=pltpu.CompilerParams(vmem_limit_bytes=60 * 2**20),
        )(seg_row, code_col, mixed, mixed, mixed)

def attn_bwd(seg_row, code_col, mixed, o, do, lse):
    rows = mixed.shape[0]; width = mixed.shape[1] // 3; pairs = width // (2 * HEAD); blocks = rows // BQ
    col, full = specs(rows)
    return pl.pallas_call(bwd_kernel, grid=(pairs,),
        in_specs=[full((1, rows)), full((rows, 1)), col(0), col(pairs), col(2 * pairs), col(0), col(0), pl.BlockSpec((1, blocks, 2 * BQ), lambda p: (p, 0, 0))],
        out_specs=[col(0), col(0), col(0)],
        out_shape=[jax.ShapeDtypeStruct((rows, width), BF16)] * 3,
        scratch_shapes=[pltpu.VMEM((slots_before(blocks, blocks) * BQ, BQ), F32), pltpu.VMEM((rows, 2 * HEAD), F32), pltpu.VMEM((rows, 2 * HEAD), F32)],
        compiler_params=pltpu.CompilerParams(vmem_limit_bytes=60 * 2**20),
        )(seg_row, code_col, mixed, mixed, mixed, o, do, lse)


def normed(values, gain_row, shift_row):
    center = values - jnp.mean(values, axis=-1, keepdims=True)
    spread = jnp.mean(center * center, axis=-1, keepdims=True)
    return center * lax.rsqrt(spread + epsilon) * gain_row + shift_row


def gelu_tanh(values):
    return 0.5 * values * (1.0 + jnp.tanh(tanh_scale * (values + 0.044715 * values * values * values)))


def transpose_dot(first_matrix, second_matrix):
    return lax.dot_general(first_matrix, second_matrix, (((0,), (0,)), ((), ())), preferred_element_type=F32)


def dot_transposed(first_matrix, second_matrix):
    return lax.dot_general(first_matrix, second_matrix, (((1,), (1,)), ((), ())), preferred_element_type=F32)


def column_sums(values):
    return jnp.sum(values.astype(F32), axis=0)


LANES = 128


def pack_rows(parts, shards):
    piece = parts[0].shape[0] // shards
    rows = jnp.concatenate([part.reshape(shards, -1, piece) for part in parts], axis=1)
    rows = jnp.pad(rows, ((0, 0), (0, 16 - rows.shape[1]), (0, LANES - piece)))
    return rows.reshape(shards * 16, LANES)


def unpack_rows(rows, piece, counts):
    table = rows.reshape(-1, 16, LANES)[:, :, :piece]
    parts, at = [], 0
    for count in counts:
        parts.append(table[:, at : at + count].reshape(-1))
        at += count
    return parts


def solution(mesh):
    by_chip = mesh.shape["dp"] == 4 and mesh.shape["fsdp"] == 8
    shards = mesh.shape["dp"] * mesh.shape["fsdp"]

    def gather_all(*arrays):
        if by_chip:
            return gather(*arrays)
        return tuple(lax.all_gather(a, AXES, axis=0, tiled=True) for a in arrays)

    def scatter_all(*arrays):
        if by_chip:
            return scatter(*arrays)
        return tuple(lax.psum_scatter(a.astype(F32), AXES, scatter_dimension=0, tiled=True) for a in arrays)

    def per_device(tokens, segment_ids, live_mask, cotangent, first_gain, first_shift, qkv_weight, query_bias, value_bias,
                   proj_weight, proj_bias, second_gain, second_shift, inner_weight, inner_bias, outer_weight, outer_bias):
        piece = first_gain.shape[0]
        vectors = (first_gain, first_shift, query_bias, value_bias, proj_bias, second_gain, second_shift, outer_bias, inner_bias)
        counts = tuple(v.shape[0] // piece for v in vectors)
        qkv, proj, inner, outer, rows = gather_all(qkv_weight, proj_weight, inner_weight, outer_weight, pack_rows(vectors, 1))
        gain_one, shift_one, qbias, vbias, pbias, gain_two, shift_two, obias, ibias = (
            v.astype(F32) for v in unpack_rows(rows, piece, counts))
        seg_row = segment_ids[None, :]
        code_col = jnp.where(live_mask == 1, segment_ids, -1)[:, None]
        wide = tokens.astype(F32)
        normed_one, first_pull = jax.vjp(normed, wide, gain_one, shift_one)
        hidden_one = normed_one.astype(BF16)
        bias_row = jnp.concatenate([qbias, jnp.zeros_like(qbias), vbias])
        mixed = (jnp.dot(hidden_one, qkv, preferred_element_type=F32) + bias_row).astype(BF16)
        attended, log_total = attn_fwd(seg_row, code_col, mixed)
        resid = wide + jnp.dot(attended, proj, preferred_element_type=F32) + pbias
        normed_two, second_pull = jax.vjp(normed, resid, gain_two, shift_two)
        hidden_two = normed_two.astype(BF16)
        pre = jnp.dot(hidden_two, inner, preferred_element_type=F32) + ibias
        act_wide, gelu_pull = jax.vjp(gelu_tanh, pre)
        act = act_wide.astype(BF16)
        layer_out = (resid + jnp.dot(act, outer, preferred_element_type=F32) + obias).astype(BF16)
        cot_wide = cotangent.astype(F32)
        grad_outer = transpose_dot(act, cotangent).astype(BF16)
        d_pre = gelu_pull(dot_transposed(cotangent, outer))[0].astype(BF16)
        grad_inner = transpose_dot(hidden_two, d_pre).astype(BF16)
        d_resid_norm, grad_gain_two, grad_shift_two = second_pull(dot_transposed(d_pre, inner))
        d_resid = cot_wide + d_resid_norm
        d_branch = d_resid.astype(BF16)
        grad_proj = transpose_dot(attended, d_branch).astype(BF16)
        d_attended = dot_transposed(d_branch, proj).astype(BF16)
        d_query, d_key, d_value = attn_bwd(seg_row, code_col, mixed, attended, d_attended, log_total)
        d_mixed = jnp.concatenate([d_query, d_key, d_value], axis=1)
        grad_qkv = transpose_dot(hidden_one, d_mixed).astype(BF16)
        d_tokens_norm, grad_gain_one, grad_shift_one = first_pull(dot_transposed(d_mixed, qkv))
        grad_tokens = (d_resid + d_tokens_norm).astype(BF16)
        sums = (grad_gain_one, grad_shift_one, column_sums(d_query), column_sums(d_value), column_sums(d_branch),
                grad_gain_two, grad_shift_two, jnp.sum(cot_wide, axis=0), column_sums(d_pre))
        s_qkv, s_proj, s_inner, s_outer, s_rows = scatter_all(
            grad_qkv, grad_proj, grad_inner, grad_outer, pack_rows(sums, shards).astype(BF16))
        g1, s1, gq, gv, gp, g2, s2, go, gi = unpack_rows(s_rows, piece, counts)
        return (layer_out, grad_tokens, g1, s1, s_qkv, gq, gv, s_proj, gp, g2, s2, s_inner, gi, s_outer, go)

    flat, matrix = P(AXES), P(AXES, None)
    return jax.shard_map(
        per_device,
        mesh=mesh,
        in_specs=(matrix, flat, flat, matrix, flat, flat, matrix, flat, flat, matrix, flat, flat, flat, matrix, flat, matrix, flat),
        out_specs=(matrix, matrix, flat, flat, matrix, flat, flat, matrix, flat, flat, flat, matrix, flat, matrix, flat),
        check_vma=False,
    )
```

```python
import jax
import jax.numpy as jnp
from jax import lax
from jax.experimental import pallas as pl
from jax.experimental.pallas import tpu as pltpu
from jax.sharding import PartitionSpec as P

D = 768
HEADS = 12
HEAD = 64
F32 = jnp.float32
BF16 = jnp.bfloat16
MESH = pl.DeviceIdType.MESH
AXES = ("dp", "fsdp")
epsilon = 1e-06
tanh_scale = 0.7978845608028654


def place():
    dp, fs = lax.axis_index("dp"), lax.axis_index("fsdp")
    return dp // 2, dp % 2, fs // 2, fs % 2

def device(x, c, z, y):
    return (x * 2 + c, z * 2 + y)

def peers(at):
    x, c, z, y = at
    return [device(x, c, (z + 1) % 4, y), device(x, c, (z + 2) % 4, y), device(x, c, (z + 3) % 4, y),
            device(x, c, z, 1 - y), device(1 - x, c, z, y), device(x, 1 - c, z, y)]

def greet(at):
    barrier = pltpu.get_barrier_semaphore()
    for peer in peers(at):
        pl.semaphore_signal(barrier, inc=1, device_id=peer, device_id_type=MESH)
    pl.semaphore_wait(barrier, 6)

def remote(src, dst, send, recv, to):
    return pltpu.make_async_remote_copy(src_ref=src, dst_ref=dst, send_sem=send, recv_sem=recv, device_id=to, device_id_type=MESH)

class Gather:
    def __init__(self, unit, at, src, out, cols, y_first, send, recv, local):
        x, c, z, y = at
        rows = src.shape[0]
        part = lambda yy: pl.ds(pl.multiple_of(yy * rows, 8), rows)
        s = lambda i: (send.at[unit, i], recv.at[unit, i])
        own = out.at[x, c, z, part(y), cols]
        self.keep = pltpu.make_async_copy(src.at[:, cols], own, local.at[unit])
        self.z = [remote(src.at[:, cols], own, *s(d), device(x, c, (z + d + 1) % 4, y)) for d in range(3)]
        line = out.at[x, c, :, part(y), cols]
        core = device(x, 1 - c, z, y)
        ydev, xdev = device(x, c, z, 1 - y), device(1 - x, c, z, y)
        if y_first:
            first, second = ydev, xdev
            got1 = out.at[x, c, :, part(1 - y), cols]
            held = out.at[x, c, :, :, cols]
            got2 = out.at[1 - x, c, :, :, cols]
        else:
            first, second = xdev, ydev
            got1 = out.at[1 - x, c, :, part(y), cols]
            held = out.at[:, c, :, part(y), cols]
            got2 = out.at[:, c, :, part(1 - y), cols]
        self.one = remote(line, line, *s(3), first)
        self.two = remote(held, held, *s(4), second)
        self.core = [remote(line, line, *s(5), core), remote(got1, got1, *s(6), core), remote(got2, got2, *s(7), core)]
    def start(self):
        self.keep.start()
        for copy in self.z:
            copy.start()
    def step1(self):
        self.keep.wait()
        for copy in self.z:
            copy.wait_recv()
        self.one.start()
        self.core[0].start()
    def step2(self):
        self.one.wait_recv()
        self.two.start()
        self.core[1].start()
    def step3(self):
        self.two.wait_recv()
        self.core[2].start()
    def arrive(self):
        for copy in self.core:
            copy.wait_recv()
    def sent(self):
        for copy in self.z + [self.one, self.two] + self.core:
            copy.wait_send()

BQ = 128
REACH = 2
NEG = -1e30

def window(block, blocks):
    return max(0, block - REACH), min(blocks, block + REACH + 1)

def nn(a, b):
    return lax.dot_general(a, b, (((1,), (0,)), ((), ())), preferred_element_type=F32)

def fill_bias(seg_row, key_code, bias_ref, blocks):
    slot = 0
    for b in range(blocks):
        low, high = window(b, blocks)
        q = seg_row[:, b * BQ:(b + 1) * BQ]
        for kb in range(low, high):
            code = key_code[kb * BQ:(kb + 1) * BQ, :]
            ok = code == q
            if kb == b:
                ok = ok | (lax.broadcasted_iota(jnp.int32, (BQ, BQ), 0) == lax.broadcasted_iota(jnp.int32, (BQ, BQ), 1))
            bias_ref[slot * BQ:(slot + 1) * BQ, :] = jnp.where(ok, 0.0, NEG)
            slot += 1

def slots_before(b, blocks):
    return sum(window(i, blocks)[1] - window(i, blocks)[0] for i in range(b))

def beside(top, low_rows):
    zero = jnp.zeros_like(top)
    return jnp.concatenate([jnp.where(low_rows, top, zero), jnp.where(low_rows, zero, top)], axis=1)

def fwd_kernel(seg_ref, code_ref, q_ref, k_ref, v_ref, o_ref, lse_ref, bias_ref):
    rows = q_ref.shape[0]
    blocks = rows // BQ
    @pl.when(pl.program_id(0) == 0)
    def _():
        fill_bias(seg_ref[...], code_ref[...], bias_ref, blocks)
    low_rows = lax.broadcasted_iota(jnp.int32, (2 * HEAD, BQ), 0) < HEAD
    vt = v_ref[...].T
    for b in range(blocks):
        low, high = window(b, blocks)
        at = slots_before(b, blocks)
        n = high - low
        qt = (q_ref[b * BQ:(b + 1) * BQ, :] * HEAD ** -0.5).T
        s = nn(k_ref[low * BQ:high * BQ, :], beside(qt, low_rows))
        bias = bias_ref[at * BQ:(at + n) * BQ, :]
        outs = []
        for h in range(2):
            sh = s[:, h * BQ:(h + 1) * BQ] + bias
            peak = jnp.max(sh, axis=0, keepdims=True)
            e = jnp.exp(sh - peak)
            total = jnp.sum(e, axis=0, keepdims=True)
            lse_ref[0, b:b + 1, h * BQ:(h + 1) * BQ] = peak + jnp.log(total)
            outs.append((e.astype(BF16), total))
        ot = nn(vt[:, low * BQ:high * BQ], jnp.concatenate([outs[0][0], outs[1][0]], axis=1))
        ot = jnp.concatenate([ot[:HEAD, :BQ] / outs[0][1], ot[HEAD:, BQ:] / outs[1][1]], axis=0)
        o_ref[b * BQ:(b + 1) * BQ, :] = ot.T.astype(BF16)

def bwd_kernel(seg_ref, code_ref, q_ref, k_ref, v_ref, o_ref, do_ref, lse_ref, dq_ref, dk_ref, dv_ref, bias_ref, dk_acc, dv_acc):
    rows = q_ref.shape[0]
    blocks = rows // BQ
    @pl.when(pl.program_id(0) == 0)
    def _():
        fill_bias(seg_ref[...], code_ref[...], bias_ref, blocks)
    low_rows = lax.broadcasted_iota(jnp.int32, (2 * HEAD, BQ), 0) < HEAD
    low_cols = lax.broadcasted_iota(jnp.int32, (BQ, 2 * HEAD), 1) < HEAD
    kt = k_ref[...].T
    dk_acc[...] = jnp.zeros_like(dk_acc)
    dv_acc[...] = jnp.zeros_like(dv_acc)
    def stack(x):
        zero = jnp.zeros_like(x)
        return jnp.concatenate([jnp.where(low_cols, x, zero), jnp.where(low_cols, zero, x)], axis=0)
    for b in range(blocks):
        low, high = window(b, blocks)
        at = slots_before(b, blocks)
        n = high - low
        here = slice(b * BQ, (b + 1) * BQ)
        q = q_ref[here, :] * HEAD ** -0.5
        do = do_ref[here, :]
        dprod = (do.astype(F32) * o_ref[here, :].astype(F32)).T
        keys = slice(low * BQ, high * BQ)
        s = nn(k_ref[keys, :], beside(q.T, low_rows))
        dp = nn(v_ref[keys, :], beside(do.T, low_rows))
        bias = bias_ref[at * BQ:(at + n) * BQ, :]
        ps, ds = [], []
        for h in range(2):
            cols = slice(h * BQ, (h + 1) * BQ)
            p = jnp.exp(s[:, cols] + bias - lse_ref[0, b:b + 1, cols])
            delta = jnp.sum(dprod[h * HEAD:(h + 1) * HEAD], axis=0, keepdims=True)
            ds.append((p * (dp[:, cols] - delta)).astype(BF16))
            ps.append(p.astype(BF16))
        p2 = jnp.concatenate(ps, axis=1)
        ds2 = jnp.concatenate(ds, axis=1)
        dv_acc[keys, :] += nn(p2, stack(do))
        dk_acc[keys, :] += nn(ds2, stack(q))
        dqt = nn(kt[:, keys], ds2)
        dqt = jnp.concatenate([dqt[:HEAD, :BQ], dqt[HEAD:, BQ:]], axis=0) * HEAD ** -0.5
        dq_ref[here, :] = dqt.T.astype(BF16)
    dk_ref[...] = dk_acc[...].astype(BF16)
    dv_ref[...] = dv_acc[...].astype(BF16)

def specs(rows):
    col = lambda off: pl.BlockSpec((rows, 2 * HEAD), lambda p: (0, p + off))
    full = lambda s: pl.BlockSpec(s, lambda p: (0,) * len(s))
    return col, full

def attn_fwd(seg_row, code_col, mixed):
    rows = mixed.shape[0]; width = mixed.shape[1] // 3; pairs = width // (2 * HEAD); blocks = rows // BQ
    col, full = specs(rows)
    return pl.pallas_call(fwd_kernel, grid=(pairs,),
        in_specs=[full((1, rows)), full((rows, 1)), col(0), col(pairs), col(2 * pairs)],
        out_specs=[col(0), pl.BlockSpec((1, blocks, 2 * BQ), lambda p: (p, 0, 0))],
        out_shape=[jax.ShapeDtypeStruct((rows, width), BF16), jax.ShapeDtypeStruct((pairs, blocks, 2 * BQ), F32)],
        scratch_shapes=[pltpu.VMEM((slots_before(blocks, blocks) * BQ, BQ), F32)],
        compiler_params=pltpu.CompilerParams(vmem_limit_bytes=60 * 2**20),
        )(seg_row, code_col, mixed, mixed, mixed)

def attn_bwd(seg_row, code_col, mixed, o, do, lse):
    rows = mixed.shape[0]; width = mixed.shape[1] // 3; pairs = width // (2 * HEAD); blocks = rows // BQ
    col, full = specs(rows)
    return pl.pallas_call(bwd_kernel, grid=(pairs,),
        in_specs=[full((1, rows)), full((rows, 1)), col(0), col(pairs), col(2 * pairs), col(0), col(0), pl.BlockSpec((1, blocks, 2 * BQ), lambda p: (p, 0, 0))],
        out_specs=[col(0), col(0), col(0)],
        out_shape=[jax.ShapeDtypeStruct((rows, width), BF16)] * 3,
        scratch_shapes=[pltpu.VMEM((slots_before(blocks, blocks) * BQ, BQ), F32), pltpu.VMEM((rows, 2 * HEAD), F32), pltpu.VMEM((rows, 2 * HEAD), F32)],
        compiler_params=pltpu.CompilerParams(vmem_limit_bytes=60 * 2**20),
        )(seg_row, code_col, mixed, mixed, mixed, o, do, lse)


def normed(values, gain_row, shift_row):
    center = values - jnp.mean(values, axis=-1, keepdims=True)
    spread = jnp.mean(center * center, axis=-1, keepdims=True)
    return center * lax.rsqrt(spread + epsilon) * gain_row + shift_row


def gelu_tanh(values):
    return 0.5 * values * (1.0 + jnp.tanh(tanh_scale * (values + 0.044715 * values * values * values)))


def transpose_dot(first_matrix, second_matrix):
    return lax.dot_general(first_matrix, second_matrix, (((0,), (0,)), ((), ())), preferred_element_type=F32)


def dot_transposed(first_matrix, second_matrix):
    return lax.dot_general(first_matrix, second_matrix, (((1,), (1,)), ((), ())), preferred_element_type=F32)


def column_sums(values):
    return jnp.sum(values.astype(F32), axis=0)


LANES = 128


VEC = 4


def norm_rows(values):
    center = values - jnp.mean(values, axis=-1, keepdims=True)
    spread = jnp.mean(center * center, axis=-1, keepdims=True)
    return center * lax.rsqrt(spread + epsilon)


def fill_masks(seg_row, code_row, bias_ref, blocks):
    slot = 0
    turned = [jnp.broadcast_to(code_row[:, b * BQ:(b + 1) * BQ], (BQ, BQ)).T for b in range(blocks)]
    for b in range(blocks):
        low, high = window(b, blocks)
        q = seg_row[:, b * BQ:(b + 1) * BQ]
        for kb in range(low, high):
            ok = turned[kb] == q
            if kb == b:
                ok = ok | (lax.broadcasted_iota(jnp.int32, (BQ, BQ), 0) == lax.broadcasted_iota(jnp.int32, (BQ, BQ), 1))
            bias_ref[slot * BQ:(slot + 1) * BQ, :] = jnp.where(ok, 0.0, NEG)
            slot += 1


def attend_block(b, blocks, q, k, vt, bias_ref, low_rows):
    low, high = window(b, blocks)
    at = slots_before(b, blocks)
    n = high - low
    s = nn(k[low * BQ:high * BQ, :], beside((q * HEAD ** -0.5).T, low_rows))
    bias = bias_ref[at * BQ:(at + n) * BQ, :]
    es, totals, logs = [], [], []
    for h in range(2):
        sh = s[:, h * BQ:(h + 1) * BQ] + bias
        peak = jnp.max(sh, axis=0, keepdims=True)
        e = jnp.exp(sh - peak)
        total = jnp.sum(e, axis=0, keepdims=True)
        es.append(e.astype(BF16))
        totals.append(total)
        logs.append(peak + jnp.log(total))
    ot = nn(vt[:, low * BQ:high * BQ], jnp.concatenate(es, axis=1))
    ot = jnp.concatenate([ot[:HEAD, :BQ] / totals[0], ot[HEAD:, BQ:] / totals[1]], axis=0)
    return ot.T.astype(BF16), jnp.concatenate(logs, axis=1)


F_UNITS = ((4, 0, 128, True), (0, 0, 1152, True), (0, 1152, 2304, False), (1, 0, 384, True), (1, 384, 768, False),
           (2, 0, 1536, True), (2, 1536, 3072, False), (3, 0, 384, True), (3, 384, 768, False))


def picker(lane_of):
    return (lax.broadcasted_iota(jnp.int32, (LANES, lane_of.shape[1]), 0) == lane_of).astype(BF16)


def spread_vectors(table, piece_of, lane_of):
    pieces, count, lanes = table.shape
    found = nn(table.reshape(pieces * count, lanes).astype(BF16), picker(lane_of))
    total = jnp.zeros((count, lane_of.shape[1]), F32)
    for d in range(pieces):
        total = total + jnp.where(piece_of == d, found[d * count:(d + 1) * count], 0.0)
    return total


def spread_vector(rows, piece_of, lane_of):
    found = nn(rows.astype(BF16), picker(lane_of))
    return jnp.sum(jnp.where(lax.broadcasted_iota(jnp.int32, found.shape, 0) == piece_of, found, 0.0), axis=0, keepdims=True)


def forward_kernel(tokens_ref, seg_ref, code_ref, piece_ref, lane_ref, wpiece_ref, wlane_ref,
                   s_qkv, s_proj, s_inner, s_outer, s_vec,
                   g_qkv, g_proj, g_inner, g_outer, ht_hbm, mixed_hbm, attended_hbm, resid_hbm, hidden_two_hbm, lse_ref, vecs_ref, ibias_ref,
                   send, recv, local, vec_buf, wide_ref, w_ref, wp_ref, bias_ref, brow_ref, hidden_ref, ht_ref, mixed_ref, attended_ref, hidden_two_ref, load):
    rows, width = tokens_ref.shape
    blocks = rows // BQ
    pairs = width // (2 * HEAD)
    at = place()
    greet(at)
    srcs, outs = (s_qkv, s_proj, s_inner, s_outer, s_vec), (g_qkv, g_proj, g_inner, g_outer, vec_buf)
    vec, q1, q2, p1, p2, n1, n2, o1, o2 = [
        Gather(u, at, srcs[k], outs[k], slice(a, b), yf, send, recv, local) for u, (k, a, b, yf) in enumerate(F_UNITS)]

    run("start", vec, q1, q2)

    @pl.loop(0, blocks)
    def _(b):
        here = pl.ds(pl.multiple_of(b * BQ, BQ), BQ)
        wide_ref[here, :] = norm_rows(tokens_ref[here, :].astype(F32))

    run("step1", vec, q1, q2)
    run("start", p1, p2, n1, n2)
    fill_masks(seg_ref[...], code_ref[...], bias_ref, blocks)
    run("step2", vec, q1, q2)
    run("step3", vec, q1, q2)
    run("arrive", vec)
    table = vec_buf[...].reshape(32, 16, LANES)
    vecs_ref[...] = spread_vectors(table, piece_ref[...], lane_ref[...])
    ibias_ref[...] = spread_vector(table[:, 8, :], wpiece_ref[...], wlane_ref[...])
    brow_ref[:, :width] = vecs_ref[2:3, :]
    brow_ref[:, width:2 * width] = jnp.zeros((1, width), F32)
    brow_ref[:, 2 * width:] = vecs_ref[3:4, :]

    @pl.loop(0, blocks)
    def _(b):
        here = pl.ds(pl.multiple_of(b * BQ, BQ), BQ)
        hidden_ref[here, :] = (wide_ref[here, :] * vecs_ref[0:1, :] + vecs_ref[1:2, :]).astype(BF16)

    ht_ref[...] = hidden_ref[...].T
    keep = [pltpu.make_async_copy(a, b, load.at[2 + i]) for i, (a, b) in enumerate((
        (ht_ref, ht_hbm), (mixed_ref, mixed_hbm), (attended_ref, attended_hbm), (wide_ref, resid_hbm), (hidden_two_ref, hidden_two_hbm)))]
    keep[0].start()
    run("arrive", q1, q2)
    fetch = pltpu.make_async_copy(g_qkv.reshape(width, 3 * width), w_ref, load.at[0])
    fetch.start()
    run("step1", p1, p2, n1, n2)
    run("start", o1, o2)
    fetch.wait()
    tile = 2 * LANES
    per = width // tile

    @pl.loop(0, 3 * per)
    def _(j):
        cols = pl.ds(pl.multiple_of(j * tile, tile), tile)
        lines = pl.ds(pl.multiple_of(j // per * rows, rows), rows)
        mixed_ref[lines, pl.ds(pl.multiple_of(j % per * tile, tile), tile)] = (nn(hidden_ref[...], w_ref[:, cols]) + brow_ref[:, cols]).astype(BF16)

        @pl.when(j == 4)
        def _():
            run("step2", p1, p2)

        @pl.when(j == 8)
        def _():
            run("step2", n1, n2)

    keep[1].start()
    low_rows = lax.broadcasted_iota(jnp.int32, (2 * HEAD, BQ), 0) < HEAD
    slots = {(0, 3): (("step3", p1, p2),), (0, 7): (("step1", o1, o2),), (1, 7): (("arrive", p1, p2), ("step3", n1, n2)),
             (3, 3): (("step2", o1, o2),), (4, 3): (("arrive", n1, n2),), (5, 3): (("step3", o1, o2),)}

    @pl.loop(0, pairs)
    def _(p):
        cols = pl.ds(pl.multiple_of(p * LANES, LANES), LANES)
        q_ref, k_ref, v_ref = [mixed_ref.at[pl.ds(part * rows, rows), cols] for part in range(3)]
        vt = v_ref[...].T
        for b in range(blocks):
            here = slice(b * BQ, (b + 1) * BQ)
            result, logs = attend_block(b, blocks, q_ref[here, :], k_ref, vt, bias_ref, low_rows)
            attended_ref[here, cols] = result
            lse_ref[p, b:b + 1, :] = logs
            for turn in range(pairs):
                if (turn, b) in slots:
                    @pl.when(p == turn)
                    def _():
                        for name, *units in slots[turn, b]:
                            run(name, *units)

    keep[2].start()
    fetch = pltpu.make_async_copy(g_proj.reshape(width, width), wp_ref, load.at[1])
    fetch.start()
    fetch.wait()

    @pl.loop(0, blocks // 2)
    def _(b):
        here = pl.ds(pl.multiple_of(b * 2 * BQ, 2 * BQ), 2 * BQ)
        resid = tokens_ref[here, :].astype(F32) + nn(attended_ref[here, :], wp_ref[...]) + vecs_ref[4:5, :]
        wide_ref[here, :] = resid
        hidden_two_ref[here, :] = (norm_rows(resid) * vecs_ref[5:6, :] + vecs_ref[6:7, :]).astype(BF16)

    keep[3].start()
    keep[4].start()
    run("arrive", o1, o2)
    for copy in keep:
        copy.wait()
    run("sent", vec, q1, q2, p1, p2, n1, n2, o1, o2)


def forward_part(tokens, seg_row, code_row, qkv, proj, inner, outer, rows16):
    rows, width = tokens.shape
    piece, ff = width // 32, inner.shape[1]
    pairs, blocks = width // (2 * HEAD), rows // BQ
    at, wide_at = jnp.arange(width, dtype=jnp.int32)[None], jnp.arange(ff, dtype=jnp.int32)[None]
    ins = (tokens, seg_row, code_row, at // piece, at % piece, wide_at // (ff // 32), wide_at % (ff // 32), qkv, proj, inner, outer, rows16)
    gathered = [jax.ShapeDtypeStruct((2, 2, 4, 2 * a.shape[0], a.shape[1]), a.dtype) for a in (qkv, proj, inner, outer)]
    made = [jax.ShapeDtypeStruct((width, rows), BF16), jax.ShapeDtypeStruct((3 * rows, width), BF16), jax.ShapeDtypeStruct((rows, width), BF16),
            jax.ShapeDtypeStruct((rows, width), F32), jax.ShapeDtypeStruct((rows, width), BF16)]
    small = [jax.ShapeDtypeStruct((pairs, blocks, 2 * BQ), F32), jax.ShapeDtypeStruct((16, width), F32), jax.ShapeDtypeStruct((1, ff), F32)]
    n = len(F_UNITS)
    out = pl.pallas_call(forward_kernel,
        out_shape=gathered + made + small,
        in_specs=[pl.BlockSpec(memory_space=pltpu.VMEM)] * len(ins),
        out_specs=[pl.BlockSpec(memory_space=pl.ANY)] * 9 + [pl.BlockSpec(memory_space=pltpu.VMEM)] * 3,
        scratch_shapes=[pltpu.SemaphoreType.DMA((n, 8)), pltpu.SemaphoreType.DMA((n, 8)), pltpu.SemaphoreType.DMA((n,)),
                        pltpu.VMEM((2, 2, 4, 32, LANES), F32), pltpu.VMEM((rows, width), F32), pltpu.VMEM((width, 3 * width), BF16),
                        pltpu.VMEM((width, width), BF16), pltpu.VMEM((slots_before(blocks, blocks) * BQ, BQ), F32), pltpu.VMEM((1, 3 * width), F32),
                        pltpu.VMEM((rows, width), BF16), pltpu.VMEM((width, rows), BF16), pltpu.VMEM((3 * rows, width), BF16), pltpu.VMEM((rows, width), BF16),
                        pltpu.VMEM((rows, width), BF16), pltpu.SemaphoreType.DMA((7,))],
        compiler_params=pltpu.CompilerParams(collective_id=0, has_side_effects=True, vmem_limit_bytes=60 * 2**20),
        name="forward_part")(*ins)
    return [g.reshape(-1, g.shape[-1]) for g in out[:4]] + list(out[4:])


CHUNK = 512


def tn(a, b):
    return lax.dot_general(a, b, (((0,), (0,)), ((), ())), preferred_element_type=F32)


def nt(a, b):
    return lax.dot_general(a, b, (((1,), (1,)), ((), ())), preferred_element_type=F32)


class Scatter:
    def __init__(self, unit, at, src, cols, x_first, bufs, send, recv, local, finish):
        x, c, z, y = at
        self.at, self.x_first, self.put = at, x_first, finish
        s = lambda i: (send.at[unit, i], recv.at[unit, i])
        self.mine, self.r0, self.r1, self.r2, self.r3 = mine, r0, r1, r2, r3 = bufs
        rows = mine.shape[3]
        grad = lambda cc, yy: src.at[:, cc, :, pl.ds(yy * rows, rows), cols]
        core, ydev, xdev = device(x, 1 - c, z, y), device(x, c, z, 1 - y), device(1 - x, c, z, y)
        self.load = [pltpu.make_async_copy(grad(c, yy), mine.at[:, :, yy], local.at[unit, yy]) for yy in range(2)]
        self.c0 = [remote(grad(1 - c, yy), r0.at[:, :, yy], *s(yy), core) for yy in range(2)]
        if x_first:
            self.c1 = remote(mine.at[1 - x], r1, *s(2), xdev)
            self.c2 = remote(mine.at[x, :, 1 - y], r2, *s(3), ydev)
        else:
            self.c1 = remote(mine.at[:, :, 1 - y], r1, *s(2), ydev)
            self.c2 = remote(mine.at[1 - x, :, y], r2, *s(3), xdev)
        self.z = [remote(mine.at[x, (z + d + 1) % 4, y], r3.at[d], *s(4 + d), device(x, c, (z + d + 1) % 4, y)) for d in range(3)]

    def start(self):
        for copy in self.c0 + self.load:
            copy.start()

    def add(self, target, other):
        target[...] = (target[...].astype(F32) + other[...].astype(F32)).astype(target.dtype)

    def step1(self):
        for copy in self.load:
            copy.wait()
        for copy in self.c0:
            copy.wait_recv()

        @pl.loop(0, 16)
        def _(j):
            i = (j // 8, (j // 2) % 4, j % 2)
            self.add(self.mine.at[i], self.r0.at[i])

        self.c1.start()

    def step2(self):
        x, c, z, y = self.at
        self.c1.wait_recv()

        @pl.loop(0, 8)
        def _(j):
            if self.x_first:
                self.add(self.mine.at[x, j // 2, j % 2], self.r1.at[j // 2, j % 2])
            else:
                self.add(self.mine.at[j // 4, j % 4, y], self.r1.at[j // 4, j % 4])

        self.c2.start()

    def step3(self):
        x, c, z, y = self.at
        self.c2.wait_recv()

        @pl.loop(0, 4)
        def _(j):
            self.add(self.mine.at[x, j, y], self.r2.at[j])

        for copy in self.z:
            copy.start()

    def finish(self):
        x, c, z, y = self.at
        for copy in self.z:
            copy.wait_recv()
        total = self.mine[x, z, y].astype(F32)
        for d in range(3):
            total = total + self.r3[d].astype(F32)
        self.put(total)

    def sent(self):
        for copy in self.c0 + [self.c1, self.c2] + self.z:
            copy.wait_send()


def run(name, *units):
    for unit in units:
        getattr(unit, name)()


def norm_back(values, grads, gain):
    center = values - jnp.mean(values, axis=-1, keepdims=True)
    r = lax.rsqrt(jnp.mean(center * center, axis=-1, keepdims=True) + epsilon)
    n = center * r
    t = grads * gain
    back = r * (t - jnp.mean(t, axis=-1, keepdims=True) - n * jnp.mean(t * n, axis=-1, keepdims=True))
    return back, jnp.sum(grads * n, axis=0, keepdims=True), jnp.sum(grads, axis=0, keepdims=True)


def backward_pair(q_ref, k_ref, v_ref, o_ref, do_ref, logs, bias_ref, dk_acc, dv_acc, blocks, low_rows, low_cols):
    kt = k_ref[...].T
    dk_acc[...] = jnp.zeros_like(dk_acc)
    dv_acc[...] = jnp.zeros_like(dv_acc)

    def stack(x):
        zero = jnp.zeros_like(x)
        return jnp.concatenate([jnp.where(low_cols, x, zero), jnp.where(low_cols, zero, x)], axis=0)

    for b in range(blocks):
        low, high = window(b, blocks)
        at = slots_before(b, blocks)
        here = slice(b * BQ, (b + 1) * BQ)
        keys = slice(low * BQ, high * BQ)
        q = q_ref[here, :] * HEAD ** -0.5
        do = do_ref[here, :]
        dprod = (do.astype(F32) * o_ref[here, :].astype(F32)).T
        s = nn(k_ref[keys, :], beside(q.T, low_rows))
        dp = nn(v_ref[keys, :], beside(do.T, low_rows))
        bias = bias_ref[at * BQ:(at + high - low) * BQ, :]
        ps, ds = [], []
        for h in range(2):
            cols = slice(h * BQ, (h + 1) * BQ)
            p = jnp.exp(s[:, cols] + bias - logs[b:b + 1, cols])
            delta = jnp.sum(dprod[h * HEAD:(h + 1) * HEAD], axis=0, keepdims=True)
            ds.append((p * (dp[:, cols] - delta)).astype(BF16))
            ps.append(p.astype(BF16))
        ds2 = jnp.concatenate(ds, axis=1)
        dv_acc[keys, :] += nn(jnp.concatenate(ps, axis=1), stack(do))
        dk_acc[keys, :] += nn(ds2, stack(q))
        dqt = nn(kt[:, keys], ds2)
        dqt = jnp.concatenate([dqt[:HEAD, :BQ], dqt[HEAD:, BQ:]], axis=0) * HEAD ** -0.5
        q_ref[here, :] = dqt.T.astype(BF16)
    k_ref[...] = dk_acc[...].astype(BF16)
    v_ref[...] = dv_acc[...].astype(BF16)


B_UNITS = tuple((2, i * CHUNK, (i + 1) * CHUNK, i % 2 == 0) for i in range(6)) + (
    (3, 0, 384, True), (3, 384, 768, False), (1, 0, 384, True), (1, 384, 768, False),
    (0, 0, 1152, True), (0, 1152, 1792, False), (0, 1792, 2304, True), (4, 0, 128, True))


def backward_kernel(seg_ref, code_ref, piece_ref, lane_ref, wpiece_ref, wlane_ref, vecs_ref, ibias_ref, lse_ref, h2_hbm, cot_hbm,
                    tokens_hbm, resid_hbm, mixed_hbm, attended_hbm, h1t_hbm, w_qkv, w_proj, w_inner, w_outer,
                    out_ref, gtok_ref, s_qkv, s_proj, s_inner, s_outer, s_vec, g_qkv, g_proj, g_inner, g_outer, g_vec,
                    send, recv, local, load, stage, h2_ref, cot_ref, a_ref, b_ref, ht_ref, acc1, acc2, resid_ref, act_ref, dpre_ref, sto, sti, att_ref,
                    bias_ref, dk_acc, dv_acc, sums, isum, vst, *bufs):
    rows, width = h2_ref.shape
    ff = ibias_ref.shape[1]
    blocks, pairs, chunks = rows // BQ, width // (2 * HEAD), ff // CHUNK
    at = place()
    greet(at)
    split = lambda ref: ref.reshape(2, 2, 4, ref.shape[0] // 16, ref.shape[1])
    grads = [split(g) for g in (g_qkv, g_proj, g_inner, g_outer)] + [g_vec]

    def put(ref, first, last):
        def write(total):
            ref[:, first:last] = total
        return write

    def put_pairs(first, last):
        def write(total):
            for tile in range(first // LANES, last // LANES):
                to = (tile % 3) * width + tile // 3 * LANES
                s_qkv[:, to:to + LANES] = total[:, tile * LANES - first:(tile + 1) * LANES - first]
        return write

    shares = (None, s_proj, s_inner, s_outer, s_vec)
    units = [Scatter(u, at, grads[k], slice(a, b), xf, bufs[5 * u:5 * u + 5], send, recv, local,
                     put_pairs(a, b) if k == 0 else put(shares[k], a, b)) for u, (k, a, b, xf) in enumerate(B_UNITS)]
    n, o, p, (q1, q2, q3), v = units[:6], units[6:8], units[8:10], units[10:13], units[13]

    tile = lambda ref, i, size: ref.at[:, pl.ds(pl.multiple_of(i * size, size), size)]
    band = lambda ref, i, size: ref.at[pl.ds(pl.multiple_of(i * size, size), size)]
    load_inner = lambda i: pltpu.make_async_copy(tile(w_inner, i, CHUNK), tile(b_ref, i, CHUNK), load.at[i])
    load_outer = lambda i: pltpu.make_async_copy(band(w_outer, i, CHUNK), band(a_ref, i, CHUNK), load.at[chunks + i])
    more = 2 * chunks
    load_resid = pltpu.make_async_copy(resid_hbm, resid_ref, load.at[more])
    load_att = pltpu.make_async_copy(attended_hbm, att_ref, load.at[more + 1])
    load_wp = pltpu.make_async_copy(w_proj, b_ref.at[:, 3 * width:], load.at[more + 2])
    load_wq = pltpu.make_async_copy(w_qkv, b_ref.at[:, :3 * width], load.at[more + 3])
    load_mixed = pltpu.make_async_copy(mixed_hbm, a_ref, load.at[more + 4])
    load_ht = pltpu.make_async_copy(h1t_hbm, ht_ref, load.at[more + 5])
    load_tok = pltpu.make_async_copy(tokens_hbm, att_ref, load.at[more + 6])
    out_inner = lambda i: pltpu.make_async_copy(sti.at[i % 2], tile(g_inner, i, CHUNK), stage.at[i % 2])
    out_outer = lambda i: pltpu.make_async_copy(sto.at[i % 2], band(g_outer, i, CHUNK), stage.at[2 + i % 2])

    load_h2 = pltpu.make_async_copy(h2_hbm, h2_ref, load.at[more + 7])
    load_cot = pltpu.make_async_copy(cot_hbm, cot_ref, load.at[more + 8])
    load_h2.start()
    load_cot.start()
    for i in range(chunks):
        load_inner(i).start()
        load_outer(i).start()
    load_resid.start()
    load_att.start()
    acc1[...] = jnp.zeros_like(acc1)
    acc2[...] = jnp.zeros_like(acc2)
    sums[...] = jnp.zeros_like(sums)
    load_h2.wait()
    ht_ref[...] = h2_ref[...].T
    load_cot.wait()
    fill_masks(seg_ref[...], code_ref[...], bias_ref, blocks)

    @pl.loop(0, chunks)
    def _(i):
        cols = pl.ds(pl.multiple_of(i * CHUNK, CHUNK), CHUNK)
        load_inner(i).wait()
        load_outer(i).wait()

        @pl.loop(0, rows // (2 * BQ))
        def _(rb):
            here = pl.ds(pl.multiple_of(rb * 2 * BQ, 2 * BQ), 2 * BQ)
            x = nn(h2_ref[here, :], b_ref[:, cols]) + ibias_ref[:, cols]
            d_act = nt(cot_ref[here, :], a_ref[cols, :])
            x2 = x * x
            half = 0.5 + 0.5 * jnp.tanh(x * (tanh_scale + tanh_scale * 0.044715 * x2))
            act = (x * half).astype(BF16)
            slope = half + half * (1.0 - half) * x * (2.0 * tanh_scale + 6.0 * tanh_scale * 0.044715 * x2)
            d_pre = (d_act * slope).astype(BF16)
            act_ref[here, :] = act
            dpre_ref[here, :] = d_pre
            acc1[here, :] += nn(act, a_ref[cols, :])
            acc2[here, :] += nt(d_pre, b_ref[:, cols])

        isum[:, cols] = jnp.sum(dpre_ref[...].astype(F32), axis=0, keepdims=True)

        @pl.when(i >= 1)
        def _():
            out_inner(i - 1).wait()
            out_outer(i - 1).wait()

        sto[i % 2] = tn(act_ref[...], cot_ref[...]).astype(BF16)
        sti[i % 2] = nn(ht_ref[...], dpre_ref[...]).astype(BF16)
        out_inner(i).start()
        out_outer(i).start()
        for turn in range(1, chunks):
            @pl.when(i == turn)
            def _():
                for name, lag in (("start", 1), ("step1", 2), ("step2", 3), ("step3", 4), ("finish", 5)):
                    if turn >= lag:
                        run(name, n[turn - lag])

    load_mixed.start()
    load_ht.start()
    load_wp.start()
    load_wq.start()
    out_inner(chunks - 1).wait()
    out_outer(chunks - 1).wait()
    run("start", n[5], *o)
    run("step1", n[4])
    run("step2", n[3])
    run("step3", n[2])
    run("finish", n[1])
    load_resid.wait()

    @pl.loop(0, blocks)
    def _(b):
        here = pl.ds(pl.multiple_of(b * BQ, BQ), BQ)
        resid = resid_ref[here, :]
        out_ref[here, :] = (resid + acc1[here, :] + vecs_ref[7:8, :]).astype(BF16)
        cot = cot_ref[here, :].astype(F32)
        back, gain, shift = norm_back(resid, acc2[here, :], vecs_ref[5:6, :])
        d_resid = cot + back
        acc1[here, :] = d_resid
        branch = d_resid.astype(BF16)
        h2_ref[here, :] = branch
        sums[4:5, :] += jnp.sum(branch.astype(F32), axis=0, keepdims=True)
        sums[5:6, :] += gain
        sums[6:7, :] += shift
        sums[7:8, :] += jnp.sum(cot, axis=0, keepdims=True)

    load_wp.wait()
    load_att.wait()

    @pl.loop(0, rows // (2 * BQ))
    def _(rb):
        here = pl.ds(pl.multiple_of(rb * 2 * BQ, 2 * BQ), 2 * BQ)
        cot_ref[here, :] = nt(h2_ref[here, :], b_ref[:, 3 * width:]).astype(BF16)

    run("step1", n[5])
    run("step2", n[4])
    run("step3", n[3])
    run("finish", n[2])
    part = tn(att_ref[...], h2_ref[...]).astype(BF16)
    sto[0, :width // 2, :] = part[:width // 2]
    sto[1, :width // 2, :] = part[width // 2:]
    out_proj = [pltpu.make_async_copy(sto.at[i, :width // 2], band(g_proj, i, width // 2), stage.at[2 + i]) for i in range(2)]
    for copy in out_proj:
        copy.start()
    run("step1", *o)
    load_mixed.wait()
    load_ht.wait()
    low_rows = lax.broadcasted_iota(jnp.int32, (2 * HEAD, BQ), 0) < HEAD
    low_cols = lax.broadcasted_iota(jnp.int32, (BQ, 2 * HEAD), 1) < HEAD
    for copy in out_proj:
        copy.wait()
    run("start", *p)
    out_pair = lambda i: pltpu.make_async_copy(sti.at[i % 2, :, :3 * LANES], tile(g_qkv, i, 3 * LANES), stage.at[i % 2])
    turns = {0: (("step2", n[5]), ("step3", n[4]), ("finish", n[3])),
             1: (("step2", *o), ("step1", *p), ("step3", n[5]), ("finish", n[4])),
             2: (("step2", *p), ("finish", n[5])),
             3: (("start", q1), ("step3", *o)),
             4: (("step1", q1), ("step3", *p), ("finish", *o)),
             5: (("step2", q1), ("finish", *p))}

    @pl.loop(0, pairs)
    def _(i):
        cols = pl.ds(pl.multiple_of(i * LANES, LANES), LANES)
        three = [a_ref.at[pl.ds(part * rows, rows), cols] for part in range(3)]
        backward_pair(*three, att_ref.at[:, cols], cot_ref.at[:, cols], lse_ref.at[i], bias_ref, dk_acc, dv_acc, blocks, low_rows, low_cols)
        sums[2:3, cols] = jnp.sum(three[0][...].astype(F32), axis=0, keepdims=True)
        sums[3:4, cols] = jnp.sum(three[2][...].astype(F32), axis=0, keepdims=True)

        @pl.when(i >= 1)
        def _():
            out_pair(i - 1).wait()

        sti[i % 2, :, :3 * LANES] = nn(ht_ref[...], jnp.concatenate([ref[...] for ref in three], axis=1)).astype(BF16)
        out_pair(i).start()
        for turn in range(pairs):
            @pl.when(i == turn)
            def _():
                for name, *some in turns[turn]:
                    run(name, *some)

    load_tok.start()
    out_pair(pairs - 1).wait()
    run("start", q2, q3)
    load_wq.wait()
    load_tok.wait()
    run("step3", q1)

    @pl.loop(0, rows // (2 * BQ))
    def _(rb):
        here = pl.ds(pl.multiple_of(rb * 2 * BQ, 2 * BQ), 2 * BQ)
        total = nt(a_ref[here, :], b_ref[:, :width])
        for part in range(1, 3):
            lines = pl.ds(pl.multiple_of(rb * 2 * BQ + part * rows, 2 * BQ), 2 * BQ)
            total = total + nt(a_ref[lines, :], b_ref[:, part * width:(part + 1) * width])
        acc2[here, :] = total

        @pl.when(rb == 2)
        def _():
            run("step1", q2, q3)

    run("step2", q2, q3)

    @pl.loop(0, blocks)
    def _(b):
        here = pl.ds(pl.multiple_of(b * BQ, BQ), BQ)
        back, gain, shift = norm_back(att_ref[here, :].astype(F32), acc2[here, :], vecs_ref[0:1, :])
        gtok_ref[here, :] = (acc1[here, :] + back).astype(BF16)
        sums[0:1, :] += gain
        sums[1:2, :] += shift

    pick, wide_pick = picker(lane_ref[...]), picker(wlane_ref[...])
    shard = lax.broadcasted_iota(jnp.int32, (32, width), 0)
    for k in range(8):
        piece = nt(jnp.where(shard == piece_ref[...], sums[k:k + 1, :], 0.0).astype(BF16), pick)
        vst[:, k, :] = piece
    shard = lax.broadcasted_iota(jnp.int32, (32, ff), 0)
    vst[:, 8, :] = nt(jnp.where(shard == wpiece_ref[...], isum[...], 0.0).astype(BF16), wide_pick)
    out_vec = pltpu.make_async_copy(vst.reshape(2, 2, 4, 32, LANES), g_vec, stage.at[0])
    out_vec.start()
    out_vec.wait()
    run("start", v)
    run("step3", q2, q3)
    run("step1", v)
    run("finish", q1)
    run("step2", v)
    run("finish", q2, q3)
    run("step3", v)
    run("finish", v)
    run("sent", *units)


def backward_part(tokens, seg_row, code_row, cotangent, qkv, proj, inner, outer, h1t, mixed, attended, log_total, resid, hidden_two, vecs, ibias):
    rows, width = tokens.shape
    ff = inner.shape[1]
    piece = width // 32
    blocks = rows // BQ
    at, wide_at = jnp.arange(width, dtype=jnp.int32)[None], jnp.arange(ff, dtype=jnp.int32)[None]
    fast = (seg_row, code_row, at // piece, at % piece, wide_at // (ff // 32), wide_at % (ff // 32), vecs, ibias, log_total)
    slow = (hidden_two, cotangent, tokens, resid, mixed, attended, h1t, qkv, proj, inner, outer)
    vmem, anywhere = pl.BlockSpec(memory_space=pltpu.VMEM), pl.BlockSpec(memory_space=pl.ANY)
    shares = [jax.ShapeDtypeStruct((a.shape[0] // 32, a.shape[1]), F32) for a in (qkv, proj, inner, outer)] + [jax.ShapeDtypeStruct((16, LANES), F32)]
    whole = [jax.ShapeDtypeStruct(a.shape, BF16) for a in (qkv, proj, inner, outer)] + [jax.ShapeDtypeStruct((2, 2, 4, 32, LANES), F32)]
    bufs = []
    for k, a, b, xf in B_UNITS:
        block = (shares[k].shape[0], b - a)
        for lead in ((2, 4, 2), (2, 4, 2), (4, 2) if xf else (2, 4), (4,), (3,)):
            bufs.append(pltpu.VMEM(lead + block, whole[k].dtype))
    n = len(B_UNITS)
    out = pl.pallas_call(backward_kernel,
        out_shape=[jax.ShapeDtypeStruct((rows, width), BF16)] * 2 + shares + whole,
        in_specs=[vmem] * len(fast) + [anywhere] * len(slow),
        out_specs=[vmem] * 7 + [anywhere] * 5,
        scratch_shapes=[pltpu.SemaphoreType.DMA((n, 7)), pltpu.SemaphoreType.DMA((n, 7)), pltpu.SemaphoreType.DMA((n, 2)), pltpu.SemaphoreType.DMA((2 * (ff // CHUNK) + 9,)), pltpu.SemaphoreType.DMA((4,)),
                        pltpu.VMEM((rows, width), BF16), pltpu.VMEM((rows, width), BF16), pltpu.VMEM((3 * rows, width), BF16), pltpu.VMEM((width, ff), BF16), pltpu.VMEM((width, rows), BF16),
                        pltpu.VMEM((rows, width), F32), pltpu.VMEM((rows, width), F32), pltpu.VMEM((rows, width), F32),
                        pltpu.VMEM((rows, CHUNK), BF16), pltpu.VMEM((rows, CHUNK), BF16), pltpu.VMEM((2, CHUNK, width), BF16), pltpu.VMEM((2, width, CHUNK), BF16),
                        pltpu.VMEM((rows, width), BF16), pltpu.VMEM((slots_before(blocks, blocks) * BQ, BQ), F32),
                        pltpu.VMEM((rows, LANES), F32), pltpu.VMEM((rows, LANES), F32), pltpu.VMEM((8, width), F32), pltpu.VMEM((1, ff), F32), pltpu.VMEM((32, 16, LANES), F32)] + bufs,
        compiler_params=pltpu.CompilerParams(collective_id=1, has_side_effects=True, vmem_limit_bytes=67043328),
        name="backward_part")(*fast, *slow)
    return out[:7]


def pack_rows(parts, shards):
    piece = parts[0].shape[0] // shards
    rows = jnp.concatenate([part.reshape(shards, -1, piece) for part in parts], axis=1)
    rows = jnp.pad(rows, ((0, 0), (0, 16 - rows.shape[1]), (0, LANES - piece)))
    return rows.reshape(shards * 16, LANES)


def unpack_rows(rows, piece, counts):
    table = rows.reshape(-1, 16, LANES)[:, :, :piece]
    parts, at = [], 0
    for count in counts:
        parts.append(table[:, at : at + count].reshape(-1))
        at += count
    return parts


def solution(mesh):
    by_chip = mesh.shape["dp"] == 4 and mesh.shape["fsdp"] == 8
    shards = mesh.shape["dp"] * mesh.shape["fsdp"]

    def gather_all(*arrays):
        return tuple(lax.all_gather(a, AXES, axis=0, tiled=True) for a in arrays)

    def scatter_all(*arrays):
        return tuple(lax.psum_scatter(a.astype(F32), AXES, scatter_dimension=0, tiled=True) for a in arrays)

    def by_kernels(tokens, segment_ids, live_mask, cotangent, qkv_weight, proj_weight, inner_weight, outer_weight, vectors):
        piece = vectors[0].shape[0]
        rows16 = jnp.stack([jnp.pad(v.astype(F32), (0, LANES - v.shape[0])) for v in vectors])
        rows16 = jnp.pad(rows16, ((0, 16 - rows16.shape[0]), (0, 0)))
        seg_row = segment_ids[None, :]
        code_row = jnp.where(live_mask == 1, segment_ids, -1)[None, :]
        qkv, proj, inner, outer, h1t, mixed, attended, resid, hidden_two, log_total, vecs, ibias = forward_part(
            tokens, seg_row, code_row, qkv_weight, proj_weight, inner_weight, outer_weight, rows16)
        layer_out, grad_tokens, s_qkv, s_proj, s_inner, s_outer, s_rows = backward_part(
            tokens, seg_row, code_row, cotangent, qkv, proj, inner, outer, h1t, mixed, attended, log_total, resid, hidden_two, vecs, ibias)
        g1, s1, gq, gv, gp, g2, s2, go = [s_rows[k, :piece] for k in range(8)]
        gi = s_rows[8, :vectors[8].shape[0]]
        return (layer_out, grad_tokens, g1, s1, s_qkv, gq, gv, s_proj, gp, g2, s2, s_inner, gi, s_outer, go)

    def per_device(tokens, segment_ids, live_mask, cotangent, first_gain, first_shift, qkv_weight, query_bias, value_bias,
                   proj_weight, proj_bias, second_gain, second_shift, inner_weight, inner_bias, outer_weight, outer_bias):
        piece = first_gain.shape[0]
        vectors = (first_gain, first_shift, query_bias, value_bias, proj_bias, second_gain, second_shift, outer_bias, inner_bias)
        counts = tuple(v.shape[0] // piece for v in vectors)
        if by_chip:
            return by_kernels(tokens, segment_ids, live_mask, cotangent, qkv_weight, proj_weight, inner_weight, outer_weight, vectors)
        qkv, proj, inner, outer, rows = gather_all(qkv_weight, proj_weight, inner_weight, outer_weight, pack_rows(vectors, 1))
        gain_one, shift_one, qbias, vbias, pbias, gain_two, shift_two, obias, ibias = (
            v.astype(F32) for v in unpack_rows(rows, piece, counts))
        seg_row = segment_ids[None, :]
        code_col = jnp.where(live_mask == 1, segment_ids, -1)[:, None]
        wide = tokens.astype(F32)
        normed_one, first_pull = jax.vjp(normed, wide, gain_one, shift_one)
        hidden_one = normed_one.astype(BF16)
        bias_row = jnp.concatenate([qbias, jnp.zeros_like(qbias), vbias])
        mixed = (jnp.dot(hidden_one, qkv, preferred_element_type=F32) + bias_row).astype(BF16)
        attended, log_total = attn_fwd(seg_row, code_col, mixed)
        resid = wide + jnp.dot(attended, proj, preferred_element_type=F32) + pbias
        normed_two, second_pull = jax.vjp(normed, resid, gain_two, shift_two)
        hidden_two = normed_two.astype(BF16)
        pre = jnp.dot(hidden_two, inner, preferred_element_type=F32) + ibias
        act_wide, gelu_pull = jax.vjp(gelu_tanh, pre)
        act = act_wide.astype(BF16)
        layer_out = (resid + jnp.dot(act, outer, preferred_element_type=F32) + obias).astype(BF16)
        cot_wide = cotangent.astype(F32)
        grad_outer = transpose_dot(act, cotangent).astype(BF16)
        d_pre = gelu_pull(dot_transposed(cotangent, outer))[0].astype(BF16)
        grad_inner = transpose_dot(hidden_two, d_pre).astype(BF16)
        d_resid_norm, grad_gain_two, grad_shift_two = second_pull(dot_transposed(d_pre, inner))
        d_resid = cot_wide + d_resid_norm
        d_branch = d_resid.astype(BF16)
        grad_proj = transpose_dot(attended, d_branch).astype(BF16)
        d_attended = dot_transposed(d_branch, proj).astype(BF16)
        d_query, d_key, d_value = attn_bwd(seg_row, code_col, mixed, attended, d_attended, log_total)
        d_mixed = jnp.concatenate([d_query, d_key, d_value], axis=1)
        grad_qkv = transpose_dot(hidden_one, d_mixed).astype(BF16)
        d_tokens_norm, grad_gain_one, grad_shift_one = first_pull(dot_transposed(d_mixed, qkv))
        grad_tokens = (d_resid + d_tokens_norm).astype(BF16)
        sums = (grad_gain_one, grad_shift_one, column_sums(d_query), column_sums(d_value), column_sums(d_branch),
                grad_gain_two, grad_shift_two, jnp.sum(cot_wide, axis=0), column_sums(d_pre))
        s_qkv, s_proj, s_inner, s_outer, s_rows = scatter_all(
            grad_qkv, grad_proj, grad_inner, grad_outer, pack_rows(sums, shards).astype(BF16))
        g1, s1, gq, gv, gp, g2, s2, go, gi = unpack_rows(s_rows, piece, counts)
        return (layer_out, grad_tokens, g1, s1, s_qkv, gq, gv, s_proj, gp, g2, s2, s_inner, gi, s_outer, go)

    flat, matrix = P(AXES), P(AXES, None)
    return jax.shard_map(
        per_device,
        mesh=mesh,
        in_specs=(matrix, flat, flat, matrix, flat, flat, matrix, flat, flat, matrix, flat, flat, flat, matrix, flat, matrix, flat),
        out_specs=(matrix, matrix, flat, flat, matrix, flat, flat, matrix, flat, flat, flat, matrix, flat, matrix, flat),
        check_vma=False,
    )
```

```python
import jax
import jax.numpy as jnp
import numpy as np
from jax import lax
from jax.experimental import pallas as pl
from jax.experimental.pallas import tpu as pltpu
from jax.sharding import PartitionSpec as P

D = 768
HEADS = 12
HEAD = 64
F32 = jnp.float32
BF16 = jnp.bfloat16
MESH = pl.DeviceIdType.MESH
AXES = ("dp", "fsdp")
epsilon = 1e-06
tanh_scale = 0.7978845608028654


def place():
    dp, fs = lax.axis_index("dp"), lax.axis_index("fsdp")
    return dp // 2, dp % 2, fs // 2, fs % 2

def device(x, c, z, y):
    return (x * 2 + c, z * 2 + y)

def peers(at):
    x, c, z, y = at
    return [device(x, c, (z + 1) % 4, y), device(x, c, (z + 2) % 4, y), device(x, c, (z + 3) % 4, y),
            device(x, c, z, 1 - y), device(1 - x, c, z, y), device(x, 1 - c, z, y)]

def greet(at):
    barrier = pltpu.get_barrier_semaphore()
    for peer in peers(at):
        pl.semaphore_signal(barrier, inc=1, device_id=peer, device_id_type=MESH)
    pl.semaphore_wait(barrier, 6)

def remote(src, dst, send, recv, to):
    return pltpu.make_async_remote_copy(src_ref=src, dst_ref=dst, send_sem=send, recv_sem=recv, device_id=to, device_id_type=MESH)

class Gather:
    def __init__(self, unit, at, src, out, cols, y_first, send, recv, local):
        x, c, z, y = at
        rows = src.shape[0]
        part = lambda yy: pl.ds(pl.multiple_of(yy * rows, 8), rows)
        s = lambda i: (send.at[unit, i], recv.at[unit, i])
        own = out.at[x, c, z, part(y), cols]
        self.keep = pltpu.make_async_copy(src.at[:, cols], own, local.at[unit])
        self.z = [remote(src.at[:, cols], own, *s(d), device(x, c, (z + d + 1) % 4, y)) for d in range(3)]
        line = out.at[x, c, :, part(y), cols]
        core = device(x, 1 - c, z, y)
        ydev, xdev = device(x, c, z, 1 - y), device(1 - x, c, z, y)
        if y_first:
            first, second = ydev, xdev
            got1 = out.at[x, c, :, part(1 - y), cols]
            held = out.at[x, c, :, :, cols]
            got2 = out.at[1 - x, c, :, :, cols]
        else:
            first, second = xdev, ydev
            got1 = out.at[1 - x, c, :, part(y), cols]
            held = out.at[:, c, :, part(y), cols]
            got2 = out.at[:, c, :, part(1 - y), cols]
        self.one = remote(line, line, *s(3), first)
        self.two = remote(held, held, *s(4), second)
        self.core = [remote(line, line, *s(5), core), remote(got1, got1, *s(6), core), remote(got2, got2, *s(7), core)]
    def start(self):
        self.keep.start()
        for copy in self.z:
            copy.start()
    def step1(self):
        self.keep.wait()
        for copy in self.z:
            copy.wait_recv()
        self.one.start()
        self.core[0].start()
    def step2(self):
        self.one.wait_recv()
        self.two.start()
        self.core[1].start()
    def step3(self):
        self.two.wait_recv()
        self.core[2].start()
    def arrive(self):
        for copy in self.core:
            copy.wait_recv()
    def sent(self):
        for copy in self.z + [self.one, self.two] + self.core:
            copy.wait_send()

BQ = 128
REACH = 2
NEG = -1e30

def window(block, blocks):
    return max(0, block - REACH), min(blocks, block + REACH + 1)

def nn(a, b):
    return lax.dot_general(a, b, (((1,), (0,)), ((), ())), preferred_element_type=F32)

def fill_bias(seg_row, key_code, bias_ref, blocks):
    slot = 0
    for b in range(blocks):
        low, high = window(b, blocks)
        q = seg_row[:, b * BQ:(b + 1) * BQ]
        for kb in range(low, high):
            code = key_code[kb * BQ:(kb + 1) * BQ, :]
            ok = code == q
            if kb == b:
                ok = ok | (lax.broadcasted_iota(jnp.int32, (BQ, BQ), 0) == lax.broadcasted_iota(jnp.int32, (BQ, BQ), 1))
            bias_ref[slot * BQ:(slot + 1) * BQ, :] = jnp.where(ok, 0.0, NEG)
            slot += 1

def slots_before(b, blocks):
    return sum(window(i, blocks)[1] - window(i, blocks)[0] for i in range(b))

def beside(top, low_rows):
    zero = jnp.zeros_like(top)
    return jnp.concatenate([jnp.where(low_rows, top, zero), jnp.where(low_rows, zero, top)], axis=1)

def fwd_kernel(seg_ref, code_ref, q_ref, k_ref, v_ref, o_ref, lse_ref, bias_ref):
    rows = q_ref.shape[0]
    blocks = rows // BQ
    @pl.when(pl.program_id(0) == 0)
    def _():
        fill_bias(seg_ref[...], code_ref[...], bias_ref, blocks)
    low_rows = lax.broadcasted_iota(jnp.int32, (2 * HEAD, BQ), 0) < HEAD
    vt = v_ref[...].T
    for b in range(blocks):
        low, high = window(b, blocks)
        at = slots_before(b, blocks)
        n = high - low
        qt = (q_ref[b * BQ:(b + 1) * BQ, :] * HEAD ** -0.5).T
        s = nn(k_ref[low * BQ:high * BQ, :], beside(qt, low_rows))
        bias = bias_ref[at * BQ:(at + n) * BQ, :]
        outs = []
        for h in range(2):
            sh = s[:, h * BQ:(h + 1) * BQ] + bias
            peak = jnp.max(sh, axis=0, keepdims=True)
            e = jnp.exp(sh - peak)
            total = jnp.sum(e, axis=0, keepdims=True)
            lse_ref[0, b:b + 1, h * BQ:(h + 1) * BQ] = peak + jnp.log(total)
            outs.append((e.astype(BF16), total))
        ot = nn(vt[:, low * BQ:high * BQ], jnp.concatenate([outs[0][0], outs[1][0]], axis=1))
        ot = jnp.concatenate([ot[:HEAD, :BQ] / outs[0][1], ot[HEAD:, BQ:] / outs[1][1]], axis=0)
        o_ref[b * BQ:(b + 1) * BQ, :] = ot.T.astype(BF16)

def bwd_kernel(seg_ref, code_ref, q_ref, k_ref, v_ref, o_ref, do_ref, lse_ref, dq_ref, dk_ref, dv_ref, bias_ref, dk_acc, dv_acc):
    rows = q_ref.shape[0]
    blocks = rows // BQ
    @pl.when(pl.program_id(0) == 0)
    def _():
        fill_bias(seg_ref[...], code_ref[...], bias_ref, blocks)
    low_rows = lax.broadcasted_iota(jnp.int32, (2 * HEAD, BQ), 0) < HEAD
    low_cols = lax.broadcasted_iota(jnp.int32, (BQ, 2 * HEAD), 1) < HEAD
    kt = k_ref[...].T
    dk_acc[...] = jnp.zeros_like(dk_acc)
    dv_acc[...] = jnp.zeros_like(dv_acc)
    def stack(x):
        zero = jnp.zeros_like(x)
        return jnp.concatenate([jnp.where(low_cols, x, zero), jnp.where(low_cols, zero, x)], axis=0)
    for b in range(blocks):
        low, high = window(b, blocks)
        at = slots_before(b, blocks)
        n = high - low
        here = slice(b * BQ, (b + 1) * BQ)
        q = q_ref[here, :] * HEAD ** -0.5
        do = do_ref[here, :]
        dprod = (do.astype(F32) * o_ref[here, :].astype(F32)).T
        keys = slice(low * BQ, high * BQ)
        s = nn(k_ref[keys, :], beside(q.T, low_rows))
        dp = nn(v_ref[keys, :], beside(do.T, low_rows))
        bias = bias_ref[at * BQ:(at + n) * BQ, :]
        ps, ds = [], []
        for h in range(2):
            cols = slice(h * BQ, (h + 1) * BQ)
            p = jnp.exp(s[:, cols] + bias - lse_ref[0, b:b + 1, cols])
            delta = jnp.sum(dprod[h * HEAD:(h + 1) * HEAD], axis=0, keepdims=True)
            ds.append((p * (dp[:, cols] - delta)).astype(BF16))
            ps.append(p.astype(BF16))
        p2 = jnp.concatenate(ps, axis=1)
        ds2 = jnp.concatenate(ds, axis=1)
        dv_acc[keys, :] += nn(p2, stack(do))
        dk_acc[keys, :] += nn(ds2, stack(q))
        dqt = nn(kt[:, keys], ds2)
        dqt = jnp.concatenate([dqt[:HEAD, :BQ], dqt[HEAD:, BQ:]], axis=0) * HEAD ** -0.5
        dq_ref[here, :] = dqt.T.astype(BF16)
    dk_ref[...] = dk_acc[...].astype(BF16)
    dv_ref[...] = dv_acc[...].astype(BF16)

def specs(rows):
    col = lambda off: pl.BlockSpec((rows, 2 * HEAD), lambda p: (0, p + off))
    full = lambda s: pl.BlockSpec(s, lambda p: (0,) * len(s))
    return col, full

def attn_fwd(seg_row, code_col, mixed):
    rows = mixed.shape[0]; width = mixed.shape[1] // 3; pairs = width // (2 * HEAD); blocks = rows // BQ
    col, full = specs(rows)
    return pl.pallas_call(fwd_kernel, grid=(pairs,),
        in_specs=[full((1, rows)), full((rows, 1)), col(0), col(pairs), col(2 * pairs)],
        out_specs=[col(0), pl.BlockSpec((1, blocks, 2 * BQ), lambda p: (p, 0, 0))],
        out_shape=[jax.ShapeDtypeStruct((rows, width), BF16), jax.ShapeDtypeStruct((pairs, blocks, 2 * BQ), F32)],
        scratch_shapes=[pltpu.VMEM((slots_before(blocks, blocks) * BQ, BQ), F32)],
        compiler_params=pltpu.CompilerParams(vmem_limit_bytes=60 * 2**20),
        )(seg_row, code_col, mixed, mixed, mixed)

def attn_bwd(seg_row, code_col, mixed, o, do, lse):
    rows = mixed.shape[0]; width = mixed.shape[1] // 3; pairs = width // (2 * HEAD); blocks = rows // BQ
    col, full = specs(rows)
    return pl.pallas_call(bwd_kernel, grid=(pairs,),
        in_specs=[full((1, rows)), full((rows, 1)), col(0), col(pairs), col(2 * pairs), col(0), col(0), pl.BlockSpec((1, blocks, 2 * BQ), lambda p: (p, 0, 0))],
        out_specs=[col(0), col(0), col(0)],
        out_shape=[jax.ShapeDtypeStruct((rows, width), BF16)] * 3,
        scratch_shapes=[pltpu.VMEM((slots_before(blocks, blocks) * BQ, BQ), F32), pltpu.VMEM((rows, 2 * HEAD), F32), pltpu.VMEM((rows, 2 * HEAD), F32)],
        compiler_params=pltpu.CompilerParams(vmem_limit_bytes=60 * 2**20),
        )(seg_row, code_col, mixed, mixed, mixed, o, do, lse)


def normed(values, gain_row, shift_row):
    center = values - jnp.mean(values, axis=-1, keepdims=True)
    spread = jnp.mean(center * center, axis=-1, keepdims=True)
    return center * lax.rsqrt(spread + epsilon) * gain_row + shift_row


def gelu_tanh(values):
    return 0.5 * values * (1.0 + jnp.tanh(tanh_scale * (values + 0.044715 * values * values * values)))


def transpose_dot(first_matrix, second_matrix):
    return lax.dot_general(first_matrix, second_matrix, (((0,), (0,)), ((), ())), preferred_element_type=F32)


def dot_transposed(first_matrix, second_matrix):
    return lax.dot_general(first_matrix, second_matrix, (((1,), (1,)), ((), ())), preferred_element_type=F32)


def column_sums(values):
    return jnp.sum(values.astype(F32), axis=0)


LANES = 128


VEC = 4


def norm_rows(values):
    center = values - jnp.mean(values, axis=-1, keepdims=True)
    spread = jnp.mean(center * center, axis=-1, keepdims=True)
    return center * lax.rsqrt(spread + epsilon)


def fill_masks(seg_row, code_row, bias_ref, blocks):
    slot = 0
    turned = [jnp.broadcast_to(code_row[:, b * BQ:(b + 1) * BQ], (BQ, BQ)).T for b in range(blocks)]
    for b in range(blocks):
        low, high = window(b, blocks)
        q = seg_row[:, b * BQ:(b + 1) * BQ]
        for kb in range(low, high):
            ok = turned[kb] == q
            if kb == b:
                ok = ok | (lax.broadcasted_iota(jnp.int32, (BQ, BQ), 0) == lax.broadcasted_iota(jnp.int32, (BQ, BQ), 1))
            bias_ref[slot * BQ:(slot + 1) * BQ, :] = jnp.where(ok, 0.0, NEG)
            slot += 1


def attend_block(b, blocks, q, k, vt, bias_ref, low_rows):
    low, high = window(b, blocks)
    at = slots_before(b, blocks)
    n = high - low
    s = nn(k[low * BQ:high * BQ, :], beside((q * HEAD ** -0.5).T, low_rows))
    bias = bias_ref[at * BQ:(at + n) * BQ, :]
    es, totals, logs = [], [], []
    for h in range(2):
        sh = s[:, h * BQ:(h + 1) * BQ] + bias
        peak = jnp.max(sh, axis=0, keepdims=True)
        e = jnp.exp(sh - peak)
        total = jnp.sum(e, axis=0, keepdims=True)
        es.append(e.astype(BF16))
        totals.append(total)
        logs.append(peak + jnp.log(total))
    ot = nn(vt[:, low * BQ:high * BQ], jnp.concatenate(es, axis=1))
    ot = jnp.concatenate([ot[:HEAD, :BQ] / totals[0], ot[HEAD:, BQ:] / totals[1]], axis=0)
    return ot.T.astype(BF16), jnp.concatenate(logs, axis=1)


F_UNITS = ((4, 0, 128, True), (0, 0, 640, True), (0, 640, 1152, False), (0, 1152, 1792, True), (0, 1792, 2304, False), (1, 0, 384, True), (1, 384, 768, False),
           (2, 0, 1536, True), (2, 1536, 3072, False), (3, 0, 384, True), (3, 384, 768, False))


def picker(lane_of):
    return (lax.broadcasted_iota(jnp.int32, (LANES, lane_of.shape[1]), 0) == lane_of).astype(BF16)


def spread_vectors(table, piece_of, lane_of):
    pieces, count, lanes = table.shape
    found = nn(table.reshape(pieces * count, lanes).astype(BF16), picker(lane_of))
    total = jnp.zeros((count, lane_of.shape[1]), F32)
    for d in range(pieces):
        total = total + jnp.where(piece_of == d, found[d * count:(d + 1) * count], 0.0)
    return total


def spread_vector(rows, piece_of, lane_of):
    found = nn(rows.astype(BF16), picker(lane_of))
    return jnp.sum(jnp.where(lax.broadcasted_iota(jnp.int32, found.shape, 0) == piece_of, found, 0.0), axis=0, keepdims=True)


def forward_kernel(tokens_ref, seg_ref, code_ref, piece_ref, lane_ref, wpiece_ref, wlane_ref,
                   s_qkv, s_proj, s_inner, s_outer, s_vec,
                   g_qkv, g_proj, g_inner, g_outer, ht_hbm, mixed_hbm, attended_hbm, resid_hbm, hidden_two_hbm, lse_ref, vecs_ref, ibias_ref,
                   send, recv, local, vec_buf, wide_ref, w_ref, wp_ref, bias_ref, brow_ref, hidden_ref, ht_ref, mixed_ref, attended_ref, hidden_two_ref, load):
    rows, width = tokens_ref.shape
    blocks = rows // BQ
    pairs = width // (2 * HEAD)
    at = place()
    greet(at)
    srcs, outs = (s_qkv, s_proj, s_inner, s_outer, s_vec), (g_qkv, g_proj, g_inner, g_outer, vec_buf)
    units = [Gather(u, at, srcs[k], outs[k], slice(a, b), yf, send, recv, local) for u, (k, a, b, yf) in enumerate(F_UNITS)]
    vec, early, late, p, n, o = units[0], units[1:3], units[3:5], units[5:7], units[7:9], units[9:11]

    run("start", vec, *early, *late)

    @pl.loop(0, blocks)
    def _(b):
        here = pl.ds(pl.multiple_of(b * BQ, BQ), BQ)
        wide_ref[here, :] = norm_rows(tokens_ref[here, :].astype(F32))

    run("step1", vec, *early)
    run("step2", vec, *early)
    run("step1", *late)
    run("start", *p, *n)
    fill_masks(seg_ref[...], code_ref[...], bias_ref, blocks)
    run("step2", *late)
    run("step3", vec, *early)
    run("arrive", vec)
    table = vec_buf[...].reshape(32, 16, LANES)
    vecs_ref[...] = spread_vectors(table, piece_ref[...], lane_ref[...])
    ibias_ref[...] = spread_vector(table[:, 8, :], wpiece_ref[...], wlane_ref[...])
    brow_ref[:, :width] = vecs_ref[2:3, :]
    brow_ref[:, width:2 * width] = jnp.zeros((1, width), F32)
    brow_ref[:, 2 * width:] = vecs_ref[3:4, :]

    @pl.loop(0, blocks)
    def _(b):
        here = pl.ds(pl.multiple_of(b * BQ, BQ), BQ)
        hidden_ref[here, :] = (wide_ref[here, :] * vecs_ref[0:1, :] + vecs_ref[1:2, :]).astype(BF16)

    ht_ref[...] = hidden_ref[...].T
    keep = [pltpu.make_async_copy(a, b, load.at[2 + i]) for i, (a, b) in enumerate((
        (ht_ref, ht_hbm), (mixed_ref, mixed_hbm), (attended_ref, attended_hbm), (wide_ref, resid_hbm), (hidden_two_ref, hidden_two_hbm)))]
    keep[0].start()
    run("step3", *late)
    run("arrive", *early, *late)
    fetch = pltpu.make_async_copy(g_qkv.reshape(width, 3 * width), w_ref, load.at[0])
    fetch.start()
    run("step1", *p, *n)
    run("start", *o)
    fetch.wait()
    tile = 2 * LANES
    per = width // tile

    @pl.loop(0, 3 * per)
    def _(j):
        cols = pl.ds(pl.multiple_of(j * tile, tile), tile)
        lines = pl.ds(pl.multiple_of(j // per * rows, rows), rows)
        mixed_ref[lines, pl.ds(pl.multiple_of(j % per * tile, tile), tile)] = (nn(hidden_ref[...], w_ref[:, cols]) + brow_ref[:, cols]).astype(BF16)

        @pl.when(j == 8)
        def _():
            run("step2", *p)

    keep[1].start()
    low_rows = lax.broadcasted_iota(jnp.int32, (2 * HEAD, BQ), 0) < HEAD
    slots = {(0, 3): (("step2", *n),), (1, 7): (("step1", *o),), (2, 3): (("step3", *p),), (4, 3): (("arrive", *p),),
             (4, 7): (("step3", *n),), (5, 3): (("step2", *o),)}

    @pl.loop(0, pairs)
    def _(pair):
        cols = pl.ds(pl.multiple_of(pair * LANES, LANES), LANES)
        q_ref, k_ref, v_ref = [mixed_ref.at[pl.ds(part * rows, rows), cols] for part in range(3)]
        vt = v_ref[...].T
        for b in range(blocks):
            here = slice(b * BQ, (b + 1) * BQ)
            result, logs = attend_block(b, blocks, q_ref[here, :], k_ref, vt, bias_ref, low_rows)
            attended_ref[here, cols] = result
            lse_ref[pair, b:b + 1, :] = logs
            for turn in range(pairs):
                if (turn, b) in slots:
                    @pl.when(pair == turn)
                    def _():
                        for name, *units in slots[turn, b]:
                            run(name, *units)

    keep[2].start()
    fetch = pltpu.make_async_copy(g_proj.reshape(width, width), wp_ref, load.at[1])
    fetch.start()
    fetch.wait()

    @pl.loop(0, blocks // 2)
    def _(b):
        here = pl.ds(pl.multiple_of(b * 2 * BQ, 2 * BQ), 2 * BQ)
        resid = tokens_ref[here, :].astype(F32) + nn(attended_ref[here, :], wp_ref[...]) + vecs_ref[4:5, :]
        wide_ref[here, :] = resid
        hidden_two_ref[here, :] = (norm_rows(resid) * vecs_ref[5:6, :] + vecs_ref[6:7, :]).astype(BF16)

    keep[3].start()
    keep[4].start()
    run("arrive", *n)
    run("step3", *o)
    run("arrive", *o)
    for copy in keep:
        copy.wait()
    run("sent", *units)


def forward_part(tokens, seg_row, code_row, qkv, proj, inner, outer, rows16):
    rows, width = tokens.shape
    piece, ff = width // 32, inner.shape[1]
    pairs, blocks = width // (2 * HEAD), rows // BQ
    at, wide_at = np.arange(width, dtype=np.int32)[None], np.arange(ff, dtype=np.int32)[None]
    ins = (tokens, seg_row, code_row, at // piece, at % piece, wide_at // (ff // 32), wide_at % (ff // 32), qkv, proj, inner, outer, rows16)
    gathered = [jax.ShapeDtypeStruct((2, 2, 4, 2 * a.shape[0], a.shape[1]), a.dtype) for a in (qkv, proj, inner, outer)]
    made = [jax.ShapeDtypeStruct((width, rows), BF16), jax.ShapeDtypeStruct((3 * rows, width), BF16), jax.ShapeDtypeStruct((rows, width), BF16),
            jax.ShapeDtypeStruct((rows, width), F32), jax.ShapeDtypeStruct((rows, width), BF16)]
    small = [jax.ShapeDtypeStruct((pairs, blocks, 2 * BQ), F32), jax.ShapeDtypeStruct((16, width), F32), jax.ShapeDtypeStruct((1, ff), F32)]
    n = len(F_UNITS)
    out = pl.pallas_call(forward_kernel,
        out_shape=gathered + made + small,
        in_specs=[pl.BlockSpec(memory_space=pltpu.VMEM)] * len(ins),
        out_specs=[pl.BlockSpec(memory_space=pl.ANY)] * 9 + [pl.BlockSpec(memory_space=pltpu.VMEM)] * 3,
        scratch_shapes=[pltpu.SemaphoreType.DMA((n, 8)), pltpu.SemaphoreType.DMA((n, 8)), pltpu.SemaphoreType.DMA((n,)),
                        pltpu.VMEM((2, 2, 4, 32, LANES), F32), pltpu.VMEM((rows, width), F32), pltpu.VMEM((width, 3 * width), BF16),
                        pltpu.VMEM((width, width), BF16), pltpu.VMEM((slots_before(blocks, blocks) * BQ, BQ), F32), pltpu.VMEM((1, 3 * width), F32),
                        pltpu.VMEM((rows, width), BF16), pltpu.VMEM((width, rows), BF16), pltpu.VMEM((3 * rows, width), BF16), pltpu.VMEM((rows, width), BF16),
                        pltpu.VMEM((rows, width), BF16), pltpu.SemaphoreType.DMA((7,))],
        compiler_params=pltpu.CompilerParams(collective_id=0, has_side_effects=True, vmem_limit_bytes=60 * 2**20),
        name="forward_part")(*ins)
    return [g.reshape(-1, g.shape[-1]) for g in out[:4]] + list(out[4:])


CHUNK = 512


def tn(a, b):
    return lax.dot_general(a, b, (((0,), (0,)), ((), ())), preferred_element_type=F32)


def nt(a, b):
    return lax.dot_general(a, b, (((1,), (1,)), ((), ())), preferred_element_type=F32)


class Scatter:
    def __init__(self, unit, at, src, cols, x_first, bufs, send, recv, local, finish):
        x, c, z, y = at
        self.at, self.x_first, self.put = at, x_first, finish
        s = lambda i: (send.at[unit, i], recv.at[unit, i])
        self.mine, self.r0, self.r1, self.r2, self.r3 = mine, r0, r1, r2, r3 = bufs
        rows = mine.shape[3]
        grad = lambda cc, yy: src.at[:, cc, :, pl.ds(yy * rows, rows), cols]
        core, ydev, xdev = device(x, 1 - c, z, y), device(x, c, z, 1 - y), device(1 - x, c, z, y)
        self.load = [pltpu.make_async_copy(grad(c, yy), mine.at[:, :, yy], local.at[unit, yy]) for yy in range(2)]
        self.c0 = [remote(grad(1 - c, yy), r0.at[:, :, yy], *s(yy), core) for yy in range(2)]
        if x_first:
            self.c1 = remote(mine.at[1 - x], r1, *s(2), xdev)
            self.c2 = remote(mine.at[x, :, 1 - y], r2, *s(3), ydev)
        else:
            self.c1 = remote(mine.at[:, :, 1 - y], r1, *s(2), ydev)
            self.c2 = remote(mine.at[1 - x, :, y], r2, *s(3), xdev)
        self.z = [remote(mine.at[x, (z + d + 1) % 4, y], r3.at[d], *s(4 + d), device(x, c, (z + d + 1) % 4, y)) for d in range(3)]

    def start(self):
        for copy in self.c0 + self.load:
            copy.start()

    def add(self, target, other):
        target[...] = target[...] + other[...]

    def step1(self):
        for copy in self.load:
            copy.wait()
        for copy in self.c0:
            copy.wait_recv()

        @pl.loop(0, 8)
        def _(j):
            self.add(self.mine.at[j // 4, j % 4], self.r0.at[j // 4, j % 4])

        self.c1.start()

    def step2(self):
        x, c, z, y = self.at
        self.c1.wait_recv()
        for i in range(4):
            if self.x_first:
                self.add(self.mine.at[x, i], self.r1.at[i])
            else:
                for j in range(2):
                    self.add(self.mine.at[j, i, y], self.r1.at[j, i])
        self.c2.start()

    def step3(self):
        x, c, z, y = self.at
        self.c2.wait_recv()
        for i in range(4):
            self.add(self.mine.at[x, i, y], self.r2.at[i])
        for copy in self.z:
            copy.start()

    def finish(self):
        x, c, z, y = self.at
        for copy in self.z:
            copy.wait_recv()
        total = self.mine[x, z, y].astype(F32)
        for d in range(3):
            total = total + self.r3[d].astype(F32)
        self.put(total)

    def sent(self):
        for copy in self.c0 + [self.c1, self.c2] + self.z:
            copy.wait_send()


def run(name, *units):
    for unit in units:
        getattr(unit, name)()


def norm_back(values, grads, gain):
    center = values - jnp.mean(values, axis=-1, keepdims=True)
    r = lax.rsqrt(jnp.mean(center * center, axis=-1, keepdims=True) + epsilon)
    n = center * r
    t = grads * gain
    back = r * (t - jnp.mean(t, axis=-1, keepdims=True) - n * jnp.mean(t * n, axis=-1, keepdims=True))
    return back, jnp.sum(grads * n, axis=0, keepdims=True), jnp.sum(grads, axis=0, keepdims=True)


def backward_pair(q_ref, k_ref, v_ref, o_ref, do_ref, logs, bias_ref, dk_acc, dv_acc, blocks, low_rows, low_cols):
    kt = k_ref[...].T
    dk_acc[...] = jnp.zeros_like(dk_acc)
    dv_acc[...] = jnp.zeros_like(dv_acc)

    def stack(x):
        zero = jnp.zeros_like(x)
        return jnp.concatenate([jnp.where(low_cols, x, zero), jnp.where(low_cols, zero, x)], axis=0)

    for b in range(blocks):
        low, high = window(b, blocks)
        at = slots_before(b, blocks)
        here = slice(b * BQ, (b + 1) * BQ)
        keys = slice(low * BQ, high * BQ)
        q = q_ref[here, :] * HEAD ** -0.5
        do = do_ref[here, :]
        dprod = (do.astype(F32) * o_ref[here, :].astype(F32)).T
        s = nn(k_ref[keys, :], beside(q.T, low_rows))
        dp = nn(v_ref[keys, :], beside(do.T, low_rows))
        bias = bias_ref[at * BQ:(at + high - low) * BQ, :]
        ps, ds = [], []
        for h in range(2):
            cols = slice(h * BQ, (h + 1) * BQ)
            p = jnp.exp(s[:, cols] + bias - logs[b:b + 1, cols])
            delta = jnp.sum(dprod[h * HEAD:(h + 1) * HEAD], axis=0, keepdims=True)
            ds.append((p * (dp[:, cols] - delta)).astype(BF16))
            ps.append(p.astype(BF16))
        ds2 = jnp.concatenate(ds, axis=1)
        dv_acc[keys, :] += nn(jnp.concatenate(ps, axis=1), stack(do))
        dk_acc[keys, :] += nn(ds2, stack(q))
        dqt = nn(kt[:, keys], ds2)
        dqt = jnp.concatenate([dqt[:HEAD, :BQ], dqt[HEAD:, BQ:]], axis=0) * HEAD ** -0.5
        q_ref[here, :] = dqt.T.astype(BF16)
    k_ref[...] = dk_acc[...].astype(BF16)
    v_ref[...] = dv_acc[...].astype(BF16)


B_UNITS = tuple((2, i * CHUNK // 2, (i + 1) * CHUNK // 2, i % 2 == 0) for i in range(12)) + (
    (3, 0, 384, True), (3, 384, 768, False), (1, 0, 384, True), (1, 384, 768, False),
    (0, 0, 640, True), (0, 640, 1152, False), (0, 1152, 1792, False), (0, 1792, 2304, True), (4, 0, 128, True))


def backward_kernel(seg_ref, code_ref, piece_ref, lane_ref, wpiece_ref, wlane_ref, vecs_ref, ibias_ref, lse_ref, h2_hbm, cot_hbm,
                    tokens_hbm, resid_hbm, mixed_hbm, attended_hbm, h1t_hbm, w_qkv, w_proj, w_inner, w_outer,
                    out_ref, gtok_ref, s_qkv, s_proj, s_inner, s_outer, s_vec, g_qkv, g_proj, g_inner, g_outer, g_vec,
                    send, recv, local, load, stage, h2_ref, cot_ref, a_ref, b_ref, ht_ref, acc1, acc2, resid_ref, act_ref, dpre_ref, sto, sti, att_ref,
                    bias_ref, dk_acc, dv_acc, sums, isum, vst, *bufs):
    rows, width = h2_ref.shape
    ff = ibias_ref.shape[1]
    blocks, pairs, chunks = rows // BQ, width // (2 * HEAD), ff // CHUNK
    at = place()
    greet(at)
    split = lambda ref: ref.reshape(2, 2, 4, ref.shape[0] // 16, ref.shape[1])
    grads = [split(g) for g in (g_qkv, g_proj, g_inner, g_outer)] + [g_vec]

    def put(ref, first, last):
        def write(total):
            ref[:, first:last] = total
        return write

    def put_pairs(first, last):
        def write(total):
            for tile in range(first // LANES, last // LANES):
                to = (tile % 3) * width + tile // 3 * LANES
                s_qkv[:, to:to + LANES] = total[:, tile * LANES - first:(tile + 1) * LANES - first]
        return write

    shares = (None, s_proj, s_inner, s_outer, s_vec)
    units = [Scatter(u, at, grads[k], slice(a, b), xf, bufs[5 * u:5 * u + 5], send, recv, local,
                     put_pairs(a, b) if k == 0 else put(shares[k], a, b)) for u, (k, a, b, xf) in enumerate(B_UNITS)]
    n, o, p, q1, q2, v = [units[i:i + 2] for i in range(0, 12, 2)], units[12:14], units[14:16], units[16:18], units[18:20], units[20]

    tile = lambda ref, i, size: ref.at[:, pl.ds(pl.multiple_of(i * size, size), size)]
    band = lambda ref, i, size: ref.at[pl.ds(pl.multiple_of(i * size, size), size)]
    load_inner = lambda i: pltpu.make_async_copy(tile(w_inner, i, CHUNK), tile(b_ref, i, CHUNK), load.at[i])
    load_outer = lambda i: pltpu.make_async_copy(band(w_outer, i, CHUNK), band(a_ref, i, CHUNK), load.at[chunks + i])
    more = 2 * chunks
    load_resid = pltpu.make_async_copy(resid_hbm, resid_ref, load.at[more])
    load_att = pltpu.make_async_copy(attended_hbm, att_ref, load.at[more + 1])
    load_wp = pltpu.make_async_copy(w_proj, b_ref.at[:, 3 * width:], load.at[more + 2])
    load_wq = pltpu.make_async_copy(w_qkv, b_ref.at[:, :3 * width], load.at[more + 3])
    load_mixed = pltpu.make_async_copy(mixed_hbm, a_ref, load.at[more + 4])
    load_ht = pltpu.make_async_copy(h1t_hbm, ht_ref, load.at[more + 5])
    load_tok = pltpu.make_async_copy(tokens_hbm, att_ref, load.at[more + 6])
    out_inner = lambda i: pltpu.make_async_copy(sti.at[i % 2], tile(g_inner, i, CHUNK), stage.at[i % 2])
    out_outer = lambda i: pltpu.make_async_copy(sto.at[i % 2], band(g_outer, i, CHUNK), stage.at[2 + i % 2])

    load_h2 = pltpu.make_async_copy(h2_hbm, h2_ref, load.at[more + 7])
    load_cot = pltpu.make_async_copy(cot_hbm, cot_ref, load.at[more + 8])
    load_h2.start()
    load_cot.start()
    for i in range(chunks):
        load_inner(i).start()
        load_outer(i).start()
    load_resid.start()
    load_att.start()
    acc1[...] = jnp.zeros_like(acc1)
    acc2[...] = jnp.zeros_like(acc2)
    sums[...] = jnp.zeros_like(sums)
    load_h2.wait()
    ht_ref[...] = h2_ref[...].T
    load_cot.wait()
    fill_masks(seg_ref[...], code_ref[...], bias_ref, blocks)

    @pl.loop(0, chunks)
    def _(i):
        cols = pl.ds(pl.multiple_of(i * CHUNK, CHUNK), CHUNK)
        load_inner(i).wait()
        load_outer(i).wait()

        @pl.loop(0, rows // (2 * BQ))
        def _(rb):
            here = pl.ds(pl.multiple_of(rb * 2 * BQ, 2 * BQ), 2 * BQ)
            x = nn(h2_ref[here, :], b_ref[:, cols]) + ibias_ref[:, cols]
            d_act = nt(cot_ref[here, :], a_ref[cols, :])
            x2 = x * x
            half = 0.5 + 0.5 * jnp.tanh(x * (tanh_scale + tanh_scale * 0.044715 * x2))
            act = (x * half).astype(BF16)
            slope = half + half * (1.0 - half) * x * (2.0 * tanh_scale + 6.0 * tanh_scale * 0.044715 * x2)
            d_pre = (d_act * slope).astype(BF16)
            act_ref[here, :] = act
            dpre_ref[here, :] = d_pre
            acc1[here, :] += nn(act, a_ref[cols, :])
            acc2[here, :] += nt(d_pre, b_ref[:, cols])

        isum[:, cols] = jnp.sum(dpre_ref[...].astype(F32), axis=0, keepdims=True)

        @pl.when(i >= 1)
        def _():
            out_inner(i - 1).wait()
            out_outer(i - 1).wait()

        sto[i % 2] = tn(act_ref[...], cot_ref[...]).astype(BF16)
        sti[i % 2] = nn(ht_ref[...], dpre_ref[...]).astype(BF16)
        out_inner(i).start()
        out_outer(i).start()
        for turn in range(1, chunks):
            @pl.when(i == turn)
            def _():
                for name, lag in (("start", 1), ("step1", 2), ("step2", 3), ("step3", 4), ("finish", 5)):
                    if turn >= lag:
                        run(name, *n[turn - lag])

    load_mixed.start()
    load_ht.start()
    load_wp.start()
    load_wq.start()
    out_inner(chunks - 1).wait()
    out_outer(chunks - 1).wait()
    run("start", *n[5], *o)
    run("step1", *n[4])
    run("step2", *n[3])
    run("step3", *n[2])
    run("finish", *n[1])
    load_resid.wait()

    @pl.loop(0, blocks)
    def _(b):
        here = pl.ds(pl.multiple_of(b * BQ, BQ), BQ)
        resid = resid_ref[here, :]
        out_ref[here, :] = (resid + acc1[here, :] + vecs_ref[7:8, :]).astype(BF16)
        cot = cot_ref[here, :].astype(F32)
        back, gain, shift = norm_back(resid, acc2[here, :], vecs_ref[5:6, :])
        d_resid = cot + back
        acc1[here, :] = d_resid
        branch = d_resid.astype(BF16)
        h2_ref[here, :] = branch
        sums[4:5, :] += jnp.sum(branch.astype(F32), axis=0, keepdims=True)
        sums[5:6, :] += gain
        sums[6:7, :] += shift
        sums[7:8, :] += jnp.sum(cot, axis=0, keepdims=True)

    load_wp.wait()
    load_att.wait()
    run("step1", *o)

    @pl.loop(0, rows // (2 * BQ))
    def _(rb):
        here = pl.ds(pl.multiple_of(rb * 2 * BQ, 2 * BQ), 2 * BQ)
        cot_ref[here, :] = nt(h2_ref[here, :], b_ref[:, 3 * width:]).astype(BF16)

    run("step1", *n[5])
    run("step2", *n[4])
    run("step3", *n[3])
    run("finish", *n[2])
    part = tn(att_ref[...], h2_ref[...]).astype(BF16)
    sto[0, :width // 2, :] = part[:width // 2]
    sto[1, :width // 2, :] = part[width // 2:]
    out_proj = [pltpu.make_async_copy(sto.at[i, :width // 2], band(g_proj, i, width // 2), stage.at[2 + i]) for i in range(2)]
    for copy in out_proj:
        copy.start()
    load_mixed.wait()
    load_ht.wait()
    low_rows = lax.broadcasted_iota(jnp.int32, (2 * HEAD, BQ), 0) < HEAD
    low_cols = lax.broadcasted_iota(jnp.int32, (BQ, 2 * HEAD), 1) < HEAD
    for copy in out_proj:
        copy.wait()
    run("start", *p)
    out_pair = lambda i: pltpu.make_async_copy(sti.at[i % 2, :, :3 * LANES], tile(g_qkv, i, 3 * LANES), stage.at[i % 2])
    turns = {0: (("step2", *n[5]), ("step3", *n[4]), ("finish", *n[3]), ("step1", *p)),
             1: (("step3", *n[5]), ("finish", *n[4])),
             2: (("step2", *o), ("finish", *n[5])),
             3: (("start", *q1), ("step2", *p)),
             4: (("step1", *q1), ("step3", *o)),
             5: (("step3", *p),)}

    @pl.loop(0, pairs)
    def _(i):
        cols = pl.ds(pl.multiple_of(i * LANES, LANES), LANES)
        three = [a_ref.at[pl.ds(part * rows, rows), cols] for part in range(3)]
        backward_pair(*three, att_ref.at[:, cols], cot_ref.at[:, cols], lse_ref.at[i], bias_ref, dk_acc, dv_acc, blocks, low_rows, low_cols)
        sums[2:3, cols] = jnp.sum(three[0][...].astype(F32), axis=0, keepdims=True)
        sums[3:4, cols] = jnp.sum(three[2][...].astype(F32), axis=0, keepdims=True)

        @pl.when(i >= 1)
        def _():
            out_pair(i - 1).wait()

        sti[i % 2, :, :3 * LANES] = nn(ht_ref[...], jnp.concatenate([ref[...] for ref in three], axis=1)).astype(BF16)
        out_pair(i).start()
        for turn in range(pairs):
            @pl.when(i == turn)
            def _():
                for name, *some in turns[turn]:
                    run(name, *some)

    load_tok.start()
    out_pair(pairs - 1).wait()
    run("start", *q2)
    load_wq.wait()
    load_tok.wait()

    @pl.loop(0, rows // (2 * BQ))
    def _(rb):
        here = pl.ds(pl.multiple_of(rb * 2 * BQ, 2 * BQ), 2 * BQ)
        total = nt(a_ref[here, :], b_ref[:, :width])
        for part in range(1, 3):
            lines = pl.ds(pl.multiple_of(rb * 2 * BQ + part * rows, 2 * BQ), 2 * BQ)
            total = total + nt(a_ref[lines, :], b_ref[:, part * width:(part + 1) * width])
        acc2[here, :] = total

        @pl.when(rb == 0)
        def _():
            run("step1", *q2)
            run("step2", *q1)

    run("step3", *q1)

    @pl.loop(0, blocks)
    def _(b):
        here = pl.ds(pl.multiple_of(b * BQ, BQ), BQ)
        back, gain, shift = norm_back(att_ref[here, :].astype(F32), acc2[here, :], vecs_ref[0:1, :])
        gtok_ref[here, :] = (acc1[here, :] + back).astype(BF16)
        sums[0:1, :] += gain
        sums[1:2, :] += shift

        @pl.when(b == blocks // 2)
        def _():
            run("step2", *q2)

    pick, wide_pick = picker(lane_ref[...]), picker(wlane_ref[...])
    shard = lax.broadcasted_iota(jnp.int32, (32, width), 0)
    for k in range(8):
        piece = nt(jnp.where(shard == piece_ref[...], sums[k:k + 1, :], 0.0).astype(BF16), pick)
        vst[:, k, :] = piece
    shard = lax.broadcasted_iota(jnp.int32, (32, ff), 0)
    vst[:, 8, :] = nt(jnp.where(shard == wpiece_ref[...], isum[...], 0.0).astype(BF16), wide_pick)
    out_vec = pltpu.make_async_copy(vst.reshape(2, 2, 4, 32, LANES), g_vec, stage.at[0])
    out_vec.start()
    out_vec.wait()
    run("start", v)
    run("step3", *q2)
    run("step1", v)
    run("finish", *p, *o)
    run("step2", v)
    run("finish", *q1)
    run("step3", v)
    run("finish", *q2, v)
    run("sent", *units)


def backward_part(tokens, seg_row, code_row, cotangent, qkv, proj, inner, outer, h1t, mixed, attended, log_total, resid, hidden_two, vecs, ibias):
    rows, width = tokens.shape
    ff = inner.shape[1]
    piece = width // 32
    blocks = rows // BQ
    at, wide_at = np.arange(width, dtype=np.int32)[None], np.arange(ff, dtype=np.int32)[None]
    fast = (seg_row, code_row, at // piece, at % piece, wide_at // (ff // 32), wide_at % (ff // 32), vecs, ibias, log_total)
    slow = (hidden_two, cotangent, tokens, resid, mixed, attended, h1t, qkv, proj, inner, outer)
    vmem, anywhere = pl.BlockSpec(memory_space=pltpu.VMEM), pl.BlockSpec(memory_space=pl.ANY)
    shares = [jax.ShapeDtypeStruct((a.shape[0] // 32, a.shape[1]), F32) for a in (qkv, proj, inner, outer)] + [jax.ShapeDtypeStruct((16, LANES), F32)]
    whole = [jax.ShapeDtypeStruct(a.shape, BF16) for a in (qkv, proj, inner, outer)] + [jax.ShapeDtypeStruct((2, 2, 4, 32, LANES), F32)]
    bufs = []
    for k, a, b, xf in B_UNITS:
        block = (shares[k].shape[0], b - a)
        for lead in ((2, 4, 2), (2, 4, 2), (4, 2) if xf else (2, 4), (4,), (3,)):
            bufs.append(pltpu.VMEM(lead + block, whole[k].dtype))
    n = len(B_UNITS)
    out = pl.pallas_call(backward_kernel,
        out_shape=[jax.ShapeDtypeStruct((rows, width), BF16)] * 2 + shares + whole,
        in_specs=[vmem] * len(fast) + [anywhere] * len(slow),
        out_specs=[vmem] * 7 + [anywhere] * 5,
        scratch_shapes=[pltpu.SemaphoreType.DMA((n, 7)), pltpu.SemaphoreType.DMA((n, 7)), pltpu.SemaphoreType.DMA((n, 2)), pltpu.SemaphoreType.DMA((2 * (ff // CHUNK) + 9,)), pltpu.SemaphoreType.DMA((4,)),
                        pltpu.VMEM((rows, width), BF16), pltpu.VMEM((rows, width), BF16), pltpu.VMEM((3 * rows, width), BF16), pltpu.VMEM((width, ff), BF16), pltpu.VMEM((width, rows), BF16),
                        pltpu.VMEM((rows, width), F32), pltpu.VMEM((rows, width), F32), pltpu.VMEM((rows, width), F32),
                        pltpu.VMEM((rows, CHUNK), BF16), pltpu.VMEM((rows, CHUNK), BF16), pltpu.VMEM((2, CHUNK, width), BF16), pltpu.VMEM((2, width, CHUNK), BF16),
                        pltpu.VMEM((rows, width), BF16), pltpu.VMEM((slots_before(blocks, blocks) * BQ, BQ), F32),
                        pltpu.VMEM((rows, LANES), F32), pltpu.VMEM((rows, LANES), F32), pltpu.VMEM((8, width), F32), pltpu.VMEM((1, ff), F32), pltpu.VMEM((32, 16, LANES), F32)] + bufs,
        compiler_params=pltpu.CompilerParams(collective_id=1, has_side_effects=True, vmem_limit_bytes=67043328),
        name="backward_part")(*fast, *slow)
    return out[:7]


def pack_rows(parts, shards):
    piece = parts[0].shape[0] // shards
    rows = jnp.concatenate([part.reshape(shards, -1, piece) for part in parts], axis=1)
    rows = jnp.pad(rows, ((0, 0), (0, 16 - rows.shape[1]), (0, LANES - piece)))
    return rows.reshape(shards * 16, LANES)


def unpack_rows(rows, piece, counts):
    table = rows.reshape(-1, 16, LANES)[:, :, :piece]
    parts, at = [], 0
    for count in counts:
        parts.append(table[:, at : at + count].reshape(-1))
        at += count
    return parts


def solution(mesh):
    by_chip = mesh.shape["dp"] == 4 and mesh.shape["fsdp"] == 8
    shards = mesh.shape["dp"] * mesh.shape["fsdp"]

    def gather_all(*arrays):
        return tuple(lax.all_gather(a, AXES, axis=0, tiled=True) for a in arrays)

    def scatter_all(*arrays):
        return tuple(lax.psum_scatter(a.astype(F32), AXES, scatter_dimension=0, tiled=True) for a in arrays)

    def by_kernels(tokens, segment_ids, live_mask, cotangent, qkv_weight, proj_weight, inner_weight, outer_weight, vectors):
        piece = vectors[0].shape[0]
        rows16 = jnp.stack([jnp.pad(v.astype(F32), (0, LANES - v.shape[0])) for v in vectors])
        rows16 = jnp.pad(rows16, ((0, 16 - rows16.shape[0]), (0, 0)))
        seg_row = segment_ids[None, :]
        code_row = jnp.where(live_mask == 1, segment_ids, -1)[None, :]
        qkv, proj, inner, outer, h1t, mixed, attended, resid, hidden_two, log_total, vecs, ibias = forward_part(
            tokens, seg_row, code_row, qkv_weight, proj_weight, inner_weight, outer_weight, rows16)
        layer_out, grad_tokens, s_qkv, s_proj, s_inner, s_outer, s_rows = backward_part(
            tokens, seg_row, code_row, cotangent, qkv, proj, inner, outer, h1t, mixed, attended, log_total, resid, hidden_two, vecs, ibias)
        g1, s1, gq, gv, gp, g2, s2, go = [s_rows[k, :piece] for k in range(8)]
        gi = s_rows[8, :vectors[8].shape[0]]
        return (layer_out, grad_tokens, g1, s1, s_qkv, gq, gv, s_proj, gp, g2, s2, s_inner, gi, s_outer, go)

    def per_device(tokens, segment_ids, live_mask, cotangent, first_gain, first_shift, qkv_weight, query_bias, value_bias,
                   proj_weight, proj_bias, second_gain, second_shift, inner_weight, inner_bias, outer_weight, outer_bias):
        piece = first_gain.shape[0]
        vectors = (first_gain, first_shift, query_bias, value_bias, proj_bias, second_gain, second_shift, outer_bias, inner_bias)
        counts = tuple(v.shape[0] // piece for v in vectors)
        if by_chip:
            return by_kernels(tokens, segment_ids, live_mask, cotangent, qkv_weight, proj_weight, inner_weight, outer_weight, vectors)
        qkv, proj, inner, outer, rows = gather_all(qkv_weight, proj_weight, inner_weight, outer_weight, pack_rows(vectors, 1))
        gain_one, shift_one, qbias, vbias, pbias, gain_two, shift_two, obias, ibias = (
            v.astype(F32) for v in unpack_rows(rows, piece, counts))
        seg_row = segment_ids[None, :]
        code_col = jnp.where(live_mask == 1, segment_ids, -1)[:, None]
        wide = tokens.astype(F32)
        normed_one, first_pull = jax.vjp(normed, wide, gain_one, shift_one)
        hidden_one = normed_one.astype(BF16)
        bias_row = jnp.concatenate([qbias, jnp.zeros_like(qbias), vbias])
        mixed = (jnp.dot(hidden_one, qkv, preferred_element_type=F32) + bias_row).astype(BF16)
        attended, log_total = attn_fwd(seg_row, code_col, mixed)
        resid = wide + jnp.dot(attended, proj, preferred_element_type=F32) + pbias
        normed_two, second_pull = jax.vjp(normed, resid, gain_two, shift_two)
        hidden_two = normed_two.astype(BF16)
        pre = jnp.dot(hidden_two, inner, preferred_element_type=F32) + ibias
        act_wide, gelu_pull = jax.vjp(gelu_tanh, pre)
        act = act_wide.astype(BF16)
        layer_out = (resid + jnp.dot(act, outer, preferred_element_type=F32) + obias).astype(BF16)
        cot_wide = cotangent.astype(F32)
        grad_outer = transpose_dot(act, cotangent).astype(BF16)
        d_pre = gelu_pull(dot_transposed(cotangent, outer))[0].astype(BF16)
        grad_inner = transpose_dot(hidden_two, d_pre).astype(BF16)
        d_resid_norm, grad_gain_two, grad_shift_two = second_pull(dot_transposed(d_pre, inner))
        d_resid = cot_wide + d_resid_norm
        d_branch = d_resid.astype(BF16)
        grad_proj = transpose_dot(attended, d_branch).astype(BF16)
        d_attended = dot_transposed(d_branch, proj).astype(BF16)
        d_query, d_key, d_value = attn_bwd(seg_row, code_col, mixed, attended, d_attended, log_total)
        d_mixed = jnp.concatenate([d_query, d_key, d_value], axis=1)
        grad_qkv = transpose_dot(hidden_one, d_mixed).astype(BF16)
        d_tokens_norm, grad_gain_one, grad_shift_one = first_pull(dot_transposed(d_mixed, qkv))
        grad_tokens = (d_resid + d_tokens_norm).astype(BF16)
        sums = (grad_gain_one, grad_shift_one, column_sums(d_query), column_sums(d_value), column_sums(d_branch),
                grad_gain_two, grad_shift_two, jnp.sum(cot_wide, axis=0), column_sums(d_pre))
        s_qkv, s_proj, s_inner, s_outer, s_rows = scatter_all(
            grad_qkv, grad_proj, grad_inner, grad_outer, pack_rows(sums, shards).astype(BF16))
        g1, s1, gq, gv, gp, g2, s2, go, gi = unpack_rows(s_rows, piece, counts)
        return (layer_out, grad_tokens, g1, s1, s_qkv, gq, gv, s_proj, gp, g2, s2, s_inner, gi, s_outer, go)

    flat, matrix = P(AXES), P(AXES, None)
    return jax.shard_map(
        per_device,
        mesh=mesh,
        in_specs=(matrix, flat, flat, matrix, flat, flat, matrix, flat, flat, matrix, flat, flat, flat, matrix, flat, matrix, flat),
        out_specs=(matrix, matrix, flat, flat, matrix, flat, flat, matrix, flat, flat, flat, matrix, flat, matrix, flat),
        check_vma=False,
    )
```
